256 devices in a mesh: blk: 128 (over x, y, z), grp: 2 (over core).
Axes of the slice: x: 4, y: 4, z: 8, core: 2. Of those that a mesh axis runs over, the one named last changes fastest.
Arguments:
- item_start: bfloat16 [32768, 128], P(('blk', 'grp')), may hold values from -0.5 to 0.5
- ratings: bfloat16 [4, 8192, 256], P(None, 'blk', 'grp'), may hold values from -6 to 6
- rating_bits: int32 [4, 8192], P(None, 'blk'), may hold values from -2147483648 to 2147483647, as said below
- plan: int32 [4], replicated, may hold values from 1 to 127, as said below
Outputs:
- user_factors: bfloat16 [8192, 128], P(('blk', 'grp'))
- item_factors: bfloat16 [32768, 128], P(('blk', 'grp'))
The draws below stay inside these ranges and needn't reach their ends.
Inputs may be any that keep to these rules, and one draw needn't show every extreme that they name: `plan`: the 4 offsets are distinct, and among them are 127 and 64. `rating_bits`: every word has a set bit among bits 0 to 15 and one among bits 16 to 31.
All inputs are finite; a program needn't handle non-finite values. Where the reference program divides by a largest or mean magnitude, that divisor is 1e-20 or more.
Results may differ from the reference program's by a relative error of at most 0.015.
Values may be sent and summed in bfloat16 or wider, within the bound.
No kernel may reach another device: no remote copies, remote signals or barrier semaphores. Data moves between devices by JAX's collectives and lax.ppermute only.
A program may use at most 64 MiB of HBM per device.

```python
import jax
import jax.numpy as jnp
from jax import lax

R = 128
UB = 64
IB = 256
KS = 4
SWEEPS = 4
NB = 128
USERS = 8192
ITEMS = 32768


def draw_rating_bits(key, part):
    shape = (KS, NB * UB)
    first_key = jax.random.fold_in(key, 11)
    second_key = jax.random.fold_in(key, 12)
    low_key = jax.random.fold_in(key, 13)
    high_key = jax.random.fold_in(key, 14)
    first_word = jax.random.randint(first_key, shape, -2147483648, 2147483647, dtype=jnp.int32)
    second_word = jax.random.randint(second_key, shape, -2147483648, 2147483647, dtype=jnp.int32)
    low_bit = jax.random.randint(low_key, shape, 0, 16, dtype=jnp.int32)
    high_bit = jax.random.randint(high_key, shape, 16, 32, dtype=jnp.int32)
    single = jnp.ones(shape, jnp.int32)
    return first_word | second_word | jnp.left_shift(single, low_bit) | jnp.left_shift(single, high_bit)


def draw_plan(key, part):
    half_block = NB // 2
    order = jax.random.permutation(jax.random.fold_in(key, 21), NB - 3).astype(jnp.int32)
    others = order[:KS - 2] + 1
    others = jnp.where(others >= half_block, others + 1, others)
    fixed_pair = jnp.array([NB - 1, half_block], dtype=jnp.int32)
    offsets = jnp.concatenate([fixed_pair, others.astype(jnp.int32)])
    placing = jax.random.permutation(jax.random.fold_in(key, 22), KS)
    return offsets[placing].astype(jnp.int32)


def block_scale(stream_key, shape, pieces, smallest, top_value):
    def one(axis_at, parts):
        heights = jax.random.uniform(jax.random.fold_in(jax.random.fold_in(stream_key, 6), axis_at), (parts,), jnp.float32, smallest / len(pieces), top_value / len(pieces))
        return jnp.repeat(jnp.exp(heights), shape[axis_at] // parts).reshape((-1,) + (1,) * (len(shape) - axis_at - 1))

    loudness = one(*pieces[0])
    for cut in pieces[1:]:
        loudness = loudness * one(*cut)
    return loudness


def centred(stream_key, extent, deviation, bound, split=(), kind=jnp.bfloat16):
    loudness = block_scale(stream_key, extent, split, -0.22, 0.18) if split else 1.0
    values = jax.random.normal(stream_key, extent, jnp.float32) * deviation * loudness
    return jnp.minimum(jnp.maximum(values, -bound), bound).astype(kind)


def setup_inputs(seed: int = 0) -> dict:
    key_of = jax.random.split(jax.random.key(seed), 5)
    item_start = centred(key_of[0], (ITEMS, R), R ** -0.5, 0.5, ((0, 256),))
    ratings = centred(key_of[1], (KS, USERS, IB), 1.0, 6.0, ((1, 128), (2, 2)))
    rating_bits = draw_rating_bits(jax.random.fold_in(key_of[4], 71), 0)
    plan = draw_plan(jax.random.fold_in(key_of[4], 71), 0)
    return {"item_start": item_start, "ratings": ratings, "rating_bits": rating_bits, "plan": plan}


ridge_scale = 0.005


def expand_bits(bitmaps, first_bit, bit_count, group_width):
    shifts = first_bit + jnp.arange(bit_count, dtype=jnp.int32)
    bit_values = jnp.right_shift(bitmaps[..., None], shifts) & 1
    spread = jnp.broadcast_to(bit_values[..., None], bit_values.shape + (group_width,))
    return spread.reshape(bitmaps.shape + (bit_count * group_width,)).astype(jnp.bfloat16)


def row_terms(indicator, rating_rows, factors):
    row_count = indicator.shape[0]
    rank_width = factors.shape[1]
    weighted = indicator[:, None, :] * factors.T[None, :, :]
    gram_sum = jnp.dot(weighted.reshape(row_count * rank_width, -1), factors, preferred_element_type=jnp.float32)
    gram_sum = gram_sum.reshape(row_count, rank_width, rank_width)
    right_side = jnp.dot(indicator * rating_rows, factors, preferred_element_type=jnp.float32)
    rated_count = jnp.sum(indicator.astype(jnp.float32), axis=1)
    return gram_sum, right_side, rated_count


def solve_rows(gram_sum, right_side, rated_count):
    rank_width = gram_sum.shape[1]
    ridge_term = ridge_scale * (rated_count + 1.0)
    identity_mat = jnp.eye(rank_width, dtype=jnp.float32)
    system = gram_sum + ridge_term[:, None, None] * identity_mat
    row_bound = jnp.max(jnp.sum(jnp.abs(system), axis=2), axis=1)
    answer = jnp.zeros_like(right_side)
    for sweep_step in range(SWEEPS):
        applied = jnp.einsum('urs,us->ur', system, answer, precision=lax.Precision.HIGHEST)
        answer = answer + (right_side - applied) / row_bound[:, None]
    return answer.astype(jnp.bfloat16)


def user_sweep(item_rows, ratings, indicators, plan):
    def solve_block(block_id):
        totals = None
        for k in range(KS):
            source = (block_id + plan[k]) % NB
            factors = lax.dynamic_slice_in_dim(item_rows, (source * IB).astype(jnp.int32), IB, 0)
            start_row = (block_id * UB).astype(jnp.int32)
            indicator = lax.dynamic_slice_in_dim(indicators[k], start_row, UB, 0)
            rating_rows = lax.dynamic_slice_in_dim(ratings[k], start_row, UB, 0)
            terms = row_terms(indicator, rating_rows, factors)
            totals = terms if totals is None else tuple(a + b for a, b in zip(totals, terms))
        return solve_rows(*totals)
    solved = lax.map(solve_block, jnp.arange(NB, dtype=jnp.int32))
    return solved.reshape(NB * UB, -1)


def item_sweep(user_rows, ratings, indicators, plan):
    def solve_block(block_id):
        totals = None
        for k in range(KS):
            source = (block_id - plan[k]) % NB
            start_row = (source * UB).astype(jnp.int32)
            factors = lax.dynamic_slice_in_dim(user_rows, start_row, UB, 0)
            indicator = lax.dynamic_slice_in_dim(indicators[k], start_row, UB, 0)
            rating_rows = lax.dynamic_slice_in_dim(ratings[k], start_row, UB, 0)
            terms = row_terms(indicator.T, rating_rows.T, factors)
            totals = terms if totals is None else tuple(a + b for a, b in zip(totals, terms))
        return solve_rows(*totals)
    solved = lax.map(solve_block, jnp.arange(NB, dtype=jnp.int32))
    return solved.reshape(NB * IB, -1)


def reference(item_start, ratings, rating_bits, plan):
    indicators = expand_bits(rating_bits, 0, 32, IB // 32)
    first_users = user_sweep(item_start, ratings, indicators, plan)
    item_factors = item_sweep(first_users, ratings, indicators, plan)
    user_factors = user_sweep(item_factors, ratings, indicators, plan)
    return user_factors, item_factors
```

```python
import functools

import jax
import jax.numpy as jnp
from jax import lax
from jax.experimental import pallas as pl
from jax.experimental.pallas import tpu as pltpu
from jax.sharding import Mesh, PartitionSpec as P

SWEEPS = 4
RIDGE = 0.005
UNRATED = 64.0
RATED_BELOW = 32.0
AXES = ("x", "y", "z")
VMEM = pltpu.MemorySpace.VMEM
SMEM = pltpu.MemorySpace.SMEM


def split_parts(value):
    high = value.astype(jnp.bfloat16)
    low = (value - high.astype(jnp.float32)).astype(jnp.bfloat16)
    return jnp.concatenate([high, low], axis=0)


def dot_f32(a, b, dims=((1,), (0,))):
    return lax.dot_general(a, b, (dims, ((), ())), preferred_element_type=jnp.float32)


def relax(right, ridge, bound, rated, factors):
    rows = right.shape[0]
    inverse = 1.0 / bound
    answer = right * inverse
    for _ in range(SWEEPS - 1):
        inner = dot_f32(split_parts(answer), factors, ((1,), (1,)))
        inner = jnp.where(rated, inner[:rows] + inner[rows:], 0.0)
        outer = dot_f32(split_parts(inner), factors)
        applied = outer[:rows] + outer[rows:] + ridge * answer
        answer = answer + (right - applied) * inverse
    return answer.astype(jnp.bfloat16)


def users_kernel(own_ref, other_ref, own_marks_ref, other_marks_ref, out_ref, factor_t_ref, mask_ref, sums_ref):
    tiles = own_ref.shape[0]
    half = own_ref.shape[1]
    rank = own_ref.shape[2]
    rows = out_ref.shape[0]
    parts = []
    marks = []
    for k in range(tiles):
        parts += [own_ref[k], other_ref[k]]
        marks += [own_marks_ref[k], other_marks_ref[k]]
    factors = jnp.concatenate(parts, axis=0)
    marked = jnp.concatenate(marks, axis=1).astype(jnp.float32)
    rated = jnp.abs(marked) < RATED_BELOW
    factor_t_ref[...] = factors.T
    mask = jnp.where(rated, 1.0, 0.0)
    mask_ref[...] = mask
    count = jnp.sum(mask, axis=1, keepdims=True)
    right = dot_f32(jnp.where(rated, marked, 0.0).astype(jnp.bfloat16), factors)

    def one(step, carry):
        for j in range(4):
            u = step * 4 + j
            row = mask_ref[pl.ds(u, 1), :].astype(jnp.bfloat16)
            gram = dot_f32(factor_t_ref[...] * row, factors)
            sums_ref[pl.ds(u, 1), :] = jnp.sum(jnp.abs(gram), axis=0, keepdims=True)
        return carry

    lax.fori_loop(0, rows // 4, one, 0)
    ridge = RIDGE * (count + 1.0)
    bound = jnp.max(sums_ref[...], axis=1, keepdims=True) + ridge
    out_ref[...] = relax(right, ridge, bound, rated, factors)


def items_kernel(own_ref, other_ref, marks_ref, out_ref, sums_ref):
    tiles = own_ref.shape[0]
    rank = own_ref.shape[2]
    items = out_ref.shape[0]
    parts = []
    for k in range(tiles):
        parts += [own_ref[k], other_ref[k]]
    factors = jnp.concatenate(parts, axis=0)
    factor_t = factors.T
    marked = jnp.concatenate([marks_ref[k].astype(jnp.float32) for k in range(tiles)], axis=0).T
    rated = jnp.abs(marked) < RATED_BELOW
    mask = jnp.where(rated, 1.0, 0.0)
    count = jnp.sum(mask, axis=1, keepdims=True)
    right = dot_f32(jnp.where(rated, marked, 0.0).astype(jnp.bfloat16), factors)
    group = 8
    for j in range(items // group):
        row = mask[j * group : j * group + 1].astype(jnp.bfloat16)
        gram = dot_f32(factor_t * row, factors)
        total = jnp.sum(jnp.abs(gram), axis=0, keepdims=True)
        sums_ref[j * group : (j + 1) * group, :] = jnp.broadcast_to(total, (group, rank))
    ridge = RIDGE * (count + 1.0)
    bound = jnp.max(sums_ref[...], axis=1, keepdims=True) + ridge
    out_ref[...] = relax(right, ridge, bound, rated, factors)


def vmem_specs(count):
    return [pl.BlockSpec(memory_space=VMEM)] * count


def solve_users(own, other, own_marks, other_marks):
    tiles, half, rank = own.shape
    rows = own_marks.shape[1]
    width = tiles * 2 * half
    return pl.pallas_call(
        users_kernel,
        out_shape=jax.ShapeDtypeStruct((rows, rank), jnp.bfloat16),
        in_specs=vmem_specs(4),
        out_specs=pl.BlockSpec(memory_space=VMEM),
        scratch_shapes=[
            pltpu.VMEM((rank, width), jnp.bfloat16),
            pltpu.VMEM((rows, width), jnp.float32),
            pltpu.VMEM((rows, rank), jnp.float32),
        ],
        name="users",
    )(own, other, own_marks, other_marks)


def solve_items(own, other, marks):
    tiles, half, rank = own.shape
    items = marks.shape[2]
    return pl.pallas_call(
        items_kernel,
        out_shape=jax.ShapeDtypeStruct((items, rank), jnp.bfloat16),
        in_specs=vmem_specs(3),
        out_specs=pl.BlockSpec(memory_space=VMEM),
        scratch_shapes=[pltpu.VMEM((items, rank), jnp.float32)],
        name="items",
    )(own, other, marks)


def pick_kernel(index_ref, source_ref, out_ref, *, units):
    for j, unit in enumerate(units):
        out_ref[j] = source_ref[index_ref[j], unit]


def pick(index, source, units):
    return pl.pallas_call(
        functools.partial(pick_kernel, units=units),
        out_shape=jax.ShapeDtypeStruct((len(units), *source.shape[2:]), source.dtype),
        in_specs=[pl.BlockSpec(memory_space=SMEM), pl.BlockSpec(memory_space=VMEM)],
        out_specs=pl.BlockSpec(memory_space=VMEM),
        name="pick",
    )(index, source)


def sent_to_all(value, axes):
    count = lax.axis_size(axes)
    copies = jnp.broadcast_to(value, (count, *value.shape))
    return lax.all_to_all(copies, axes, split_axis=0, concat_axis=0, tiled=True)


def fetched_from(value, axis, steps):
    count = lax.axis_size(axis)
    return lax.ppermute(value, axis, [((target + steps) % count, target) for target in range(count)])


def shift_digits(shift):
    nz, ny, nx = lax.axis_size("z"), lax.axis_size("y"), lax.axis_size("x")
    z = lax.axis_index("z") + shift % nz
    y_step = (shift // nz) % ny + z // nz
    y = lax.axis_index("y") + y_step
    x_step = shift // (nz * ny) + y // ny
    return z % nz, y_step % ny, x_step % nx


def fetch(value, source_units, digits):
    z_at, y_step, x_step = digits
    held = pick(z_at, sent_to_all(value, "z"), source_units)
    for axis, steps in (("y", y_step), ("x", x_step)):
        chosen = held
        for step in range(1, lax.axis_size(axis)):
            arrived = fetched_from(held, axis, step)
            chosen = jnp.where((steps == step)[:, None, None], arrived, chosen)
        held = chosen
    return held


def body(item_start, ratings, rating_bits, plan):
    tiles, users, items = ratings.shape
    rank = item_start.shape[1]
    own_half = lax.axis_index("grp")
    blocks = lax.axis_size(AXES)
    rows = users // 2
    partner = lambda value: fetched_from(value, "grp", 1)

    bit_count = 32 // lax.axis_size("grp")
    item_bits = own_half * bit_count + lax.broadcasted_iota(jnp.int32, (1, 1, items), 2) // (items // bit_count)
    rated = (jnp.right_shift(rating_bits[:, :, None], item_bits) & 1) == 1
    marks = jnp.where(rated, ratings, jnp.asarray(UNRATED, ratings.dtype))
    swapped = jnp.concatenate([marks[:, rows:], marks[:, :rows]], axis=1)
    marks = jnp.where(own_half == 0, marks, swapped)
    own_marks = marks[:, :rows]
    other_marks = partner(marks[:, rows:])

    forward = shift_digits(plan)
    backward = shift_digits((blocks - plan) % blocks)
    twice = lambda digits: tuple(jnp.repeat(d, 2) for d in digits)
    item_units = item_start.shape[0] // users

    value = jnp.concatenate([item_start.reshape(item_units, users, rank), marks], axis=0)
    units = [u for k in range(tiles) for u in range(item_units)] + [item_units + k for k in range(tiles)]
    both = tuple(jnp.concatenate([jnp.repeat(f, item_units), b]) for f, b in zip(forward, backward))
    arrived = fetch(value, units, both)
    own_items = arrived[: tiles * item_units].reshape(tiles, -1, rank)
    moved_marks = arrived[tiles * item_units :]
    first_users = solve_users(own_items, partner(own_items), own_marks, other_marks)

    own_users = fetch(first_users[None], [0] * tiles, backward)
    item_factors = solve_items(own_users, partner(own_users), moved_marks)

    own_items = fetch(item_factors[None], [0] * tiles, forward)
    user_factors = solve_users(own_items, partner(own_items), own_marks, other_marks)
    return (user_factors, item_factors)


def solution(mesh):
    torus = Mesh(mesh.devices.reshape(4, 4, 8, 2), (*AXES, "grp"))
    everywhere = (*AXES, "grp")
    in_specs = (P(everywhere, None), P(None, AXES, "grp"), P(None, AXES), P())
    out_specs = (P(everywhere, None), P(everywhere, None))
    return jax.shard_map(body, mesh=torus, in_specs=in_specs, out_specs=out_specs, check_vma=False)
```

```python
import functools

import jax
import jax.numpy as jnp
from jax import lax
from jax.experimental import pallas as pl
from jax.experimental.pallas import tpu as pltpu
from jax.sharding import Mesh, PartitionSpec as P

SWEEPS = 4
RIDGE = 0.005
UNRATED = 64.0
RATED_BELOW = 32.0
AXES = ("x", "y", "z")
VMEM = pltpu.MemorySpace.VMEM
SMEM = pltpu.MemorySpace.SMEM


def split_parts(value):
    high = value.astype(jnp.bfloat16)
    low = (value - high.astype(jnp.float32)).astype(jnp.bfloat16)
    return jnp.concatenate([high, low], axis=0)


def dot_f32(a, b, dims=((1,), (0,))):
    return lax.dot_general(a, b, (dims, ((), ())), preferred_element_type=jnp.float32)


def relax(right, ridge, bound, rated, factors):
    rows = right.shape[0]
    inverse = 1.0 / bound
    answer = right * inverse
    for _ in range(SWEEPS - 1):
        inner = dot_f32(split_parts(answer), factors, ((1,), (1,)))
        inner = jnp.where(rated, inner[:rows] + inner[rows:], 0.0)
        outer = dot_f32(split_parts(inner), factors)
        applied = outer[:rows] + outer[rows:] + ridge * answer
        answer = answer + (right - applied) * inverse
    return answer.astype(jnp.bfloat16)


def users_kernel(*refs, static, copies, extra):
    refs = list(refs)
    own = [refs.pop(0) for _ in range(static + 1)]
    other = [refs.pop(0) for _ in range(static + 1)]
    own_marks_ref, other_marks_ref = refs.pop(0), refs.pop(0)
    extra_ref = refs.pop(0) if extra else None
    out_ref, factor_t_ref, mask_ref, sums_ref = refs
    rank = own[0].shape[1]
    rows = own_marks_ref.shape[1]
    parts = []
    for k in range(static):
        parts += [own[k][...], other[k][...]]
    for k in range(own[static].shape[0]):
        parts += [own[static][k], other[static][k]]
    marks = []
    for k in range(own_marks_ref.shape[0]):
        marks += [own_marks_ref[k], other_marks_ref[k]]
    factors = jnp.concatenate(parts, axis=0)
    marked = jnp.concatenate(marks, axis=1).astype(jnp.float32)
    rated = jnp.abs(marked) < RATED_BELOW
    factor_t_ref[...] = factors.T
    mask = jnp.where(rated, 1.0, 0.0)
    mask_ref[...] = mask
    count = jnp.sum(mask, axis=1, keepdims=True)
    right = dot_f32(jnp.where(rated, marked, 0.0).astype(jnp.bfloat16), factors)
    together = 16

    def some(step, carry):
        chosen = mask_ref[pl.ds(step * together, together), :].astype(jnp.bfloat16)
        weighted = (factor_t_ref[...][None] * chosen[:, None, :]).reshape(together * rank, -1)
        gram = dot_f32(weighted, factors)
        total = jnp.sum(jnp.abs(gram).reshape(together, rank, rank), axis=1)
        sums_ref[pl.ds(step * together, together), :] = total
        return carry

    lax.fori_loop(0, rows // together, some, 0)
    ridge = RIDGE * (count + 1.0)
    bound = jnp.max(sums_ref[...], axis=1, keepdims=True) + ridge
    answer = relax(right, ridge, bound, rated, factors)
    if not copies:
        out_ref[...] = answer
    for c in range(copies):
        out_ref[c, :rows, :] = answer
        for k in range(extra_ref.shape[0] if extra else 0):
            start = rows + k * extra_ref.shape[1]
            out_ref[c, start : start + extra_ref.shape[1], :] = extra_ref[k]


def items_kernel(own_ref, other_ref, *refs, static, copies):
    marks_refs, (out_ref, copies_ref, sums_ref) = refs[: static + 1], refs[static + 1 :]
    tiles = own_ref.shape[0]
    rank = own_ref.shape[2]
    items = out_ref.shape[0]
    parts = []
    for k in range(tiles):
        parts += [own_ref[k], other_ref[k]]
    factors = jnp.concatenate(parts, axis=0)
    factor_t = factors.T
    marks = [ref[...] for ref in marks_refs[:static]]
    marks += [marks_refs[static][k] for k in range(marks_refs[static].shape[0])]
    marked = jnp.concatenate([m.astype(jnp.float32) for m in marks], axis=0).T
    rated = jnp.abs(marked) < RATED_BELOW
    mask = jnp.where(rated, 1.0, 0.0)
    count = jnp.sum(mask, axis=1, keepdims=True)
    right = dot_f32(jnp.where(rated, marked, 0.0).astype(jnp.bfloat16), factors)
    group = 8
    for j in range(items // group):
        row = mask[j * group : j * group + 1].astype(jnp.bfloat16)
        gram = dot_f32(factor_t * row, factors)
        total = jnp.sum(jnp.abs(gram), axis=0, keepdims=True)
        sums_ref[j * group : (j + 1) * group, :] = jnp.broadcast_to(total, (group, rank))
    ridge = RIDGE * (count + 1.0)
    bound = jnp.max(sums_ref[...], axis=1, keepdims=True) + ridge
    answer = relax(right, ridge, bound, rated, factors)
    out_ref[...] = answer
    for c in range(copies):
        copies_ref[c] = answer


def vmem_specs(count):
    return [pl.BlockSpec(memory_space=VMEM)] * count


def solve_users(own, other, own_marks, other_marks, copies=0, extra=None):
    static = len(own) - 1
    tiles, rows, half = own_marks.shape
    rank = own[0].shape[1]
    width = tiles * 2 * half
    args = [*own, *other, own_marks, other_marks]
    shape = (rows, rank)
    if copies:
        args.append(extra)
        shape = (copies, rows + extra.shape[0] * extra.shape[1], rank)
    return pl.pallas_call(
        functools.partial(users_kernel, static=static, copies=copies, extra=copies > 0),
        out_shape=jax.ShapeDtypeStruct(shape, jnp.bfloat16),
        in_specs=vmem_specs(len(args)),
        out_specs=pl.BlockSpec(memory_space=VMEM),
        scratch_shapes=[
            pltpu.VMEM((rank, width), jnp.bfloat16),
            pltpu.VMEM((rows, width), jnp.float32),
            pltpu.VMEM((rows, rank), jnp.float32),
        ],
        name="users",
    )(*args)


def solve_items(own, other, marks, copies):
    tiles, half, rank = own.shape
    items = marks[0].shape[1]
    return pl.pallas_call(
        functools.partial(items_kernel, static=len(marks) - 1, copies=copies),
        out_shape=(
            jax.ShapeDtypeStruct((items, rank), jnp.bfloat16),
            jax.ShapeDtypeStruct((copies, items, rank), jnp.bfloat16),
        ),
        in_specs=vmem_specs(2 + len(marks)),
        out_specs=tuple(vmem_specs(2)),
        scratch_shapes=[pltpu.VMEM((items, rank), jnp.float32)],
        name="items",
    )(own, other, *marks)


def small_call(kernel, name, index, arrays, out_shapes):
    return pl.pallas_call(
        kernel,
        out_shape=tuple(jax.ShapeDtypeStruct(shape, jnp.bfloat16) for shape in out_shapes),
        in_specs=[pl.BlockSpec(memory_space=SMEM)] + vmem_specs(len(arrays)),
        out_specs=tuple(vmem_specs(len(out_shapes))),
        name=name,
    )(index, *arrays)


def arrange_kernel(index_ref, marks_ref, out_ref):
    tiles, users, _ = marks_ref.shape
    rows = users // 2
    half = index_ref[tiles]
    for k in range(tiles):
        for part, at in ((0, half), (1, 1 - half)):
            start = pl.multiple_of(at * rows, rows)
            out_ref[k, part * rows : (part + 1) * rows, :] = marks_ref[index_ref[k], pl.ds(start, rows), :]


def pick_kernel(index_ref, source_ref, out_ref):
    for k in range(out_ref.shape[0]):
        out_ref[k] = source_ref[index_ref[k]]


def pick_items_kernel(index_ref, source_ref, marks_ref, out_ref):
    tiles, users, _ = marks_ref.shape
    for k in range(tiles):
        for unit in range(source_ref.shape[1] // users):
            out_ref[k * (source_ref.shape[1] // users) + unit] = source_ref[
                index_ref[k], unit * users : (unit + 1) * users, :
            ]
        out_ref[out_ref.shape[0] - tiles + k] = marks_ref[k]


def pick_users_kernel(index_ref, source_ref, copies_ref, marks_ref):
    copies, tiles, rows, _ = copies_ref.shape
    for k in range(tiles):
        piece = source_ref[index_ref[k], :rows, :]
        for c in range(copies):
            copies_ref[c, k] = piece
    first = tiles - marks_ref.shape[0]
    users = marks_ref.shape[1]
    for k in range(marks_ref.shape[0]):
        marks_ref[k] = source_ref[index_ref[first + k], rows + k * users : rows + (k + 1) * users, :]


def pick_own_kernel(index_ref, source_ref, out_ref):
    for k in range(out_ref.shape[0]):
        out_ref[k] = source_ref[index_ref[k], k]


def swapped_with_all(copies, axes):
    return lax.all_to_all(copies, axes, split_axis=0, concat_axis=0, tiled=True)


def fetched_from(value, axis, steps):
    count = 1
    for name in (axis if isinstance(axis, tuple) else (axis,)):
        count *= lax.axis_size(name)
    return lax.ppermute(value, axis, [((target + steps) % count, target) for target in range(count)])


def shift_digits(shift, z_first):
    nz, ny, nx = lax.axis_size("z"), lax.axis_size("y"), lax.axis_size("x")
    z, z_shift = lax.axis_index("z"), shift % nz
    carry = (z + z_shift) // nz if z_first else (z < z_shift).astype(jnp.int32)
    y_step = (shift // nz) % ny + carry
    x_step = shift // (nz * ny) + (lax.axis_index("y") + y_step) // ny
    return (z + z_shift) % nz, y_step % ny, x_step % nx


def stepped(held, axis, steps):
    chosen = held
    for step in range(1, lax.axis_size(axis)):
        arrived = fetched_from(held, axis, step)
        chosen = jnp.where((steps == step)[:, None, None], arrived, chosen)
    return chosen


def body(item_start, ratings, rating_bits, plan):
    tiles, users, items = ratings.shape
    rank = item_start.shape[1]
    own_half = lax.axis_index("grp")
    blocks = lax.axis_size(AXES)
    nz, ny, nx = lax.axis_size("z"), lax.axis_size("y"), lax.axis_size("x")
    rows = users // 2
    partner = lambda value: fetched_from(value, "grp", 1)

    fixed = (blocks - 1, blocks // 2)
    rank_of = jnp.where(plan == fixed[0], 0, jnp.where(plan == fixed[1], 1, 2))
    before = (rank_of[None, :] < rank_of[:, None]) | (
        (rank_of[None, :] == rank_of[:, None]) & (jnp.arange(tiles)[None, :] < jnp.arange(tiles)[:, None])
    )
    place = jnp.sum(before.astype(jnp.int32), axis=1)
    at_place = (place[None, :] == jnp.arange(tiles)[:, None]).astype(jnp.int32)
    order = jnp.sum(at_place * jnp.arange(tiles)[None, :], axis=1)
    shifts = jnp.sum(at_place * plan[None, :], axis=1)
    moving = shifts[len(fixed) :]
    moves = tiles - len(fixed)
    z_items, y_items, x_items = shift_digits(moving, True)
    _, y_marks, x_marks = shift_digits((blocks - moving) % blocks, False)
    z_users, y_users, x_users = shift_digits((blocks - shifts) % blocks, True)
    x_users = (lax.axis_index("x") + x_users) % nx
    y_users = (lax.axis_index("y") + y_users) % ny

    bit_count = 32 // lax.axis_size("grp")
    item_bits = own_half * bit_count + lax.broadcasted_iota(jnp.int32, (1, 1, items), 2) // (items // bit_count)
    rated = (jnp.right_shift(rating_bits[:, :, None], item_bits) & 1) == 1
    marks = jnp.where(rated, ratings, jnp.asarray(UNRATED, ratings.dtype))
    index = jnp.concatenate([order, own_half[None]])
    (marks,) = small_call(arrange_kernel, "arrange", index, [marks], [marks.shape])
    own_marks = marks[:, :rows]
    other_marks = partner(marks[:, rows:])
    fixed_marks = [fetched_from(marks[k], AXES, -fixed[k]) for k in range(len(fixed))]

    def gather_items(factors, copies, extra):
        fixed_own = [fetched_from(factors, AXES, shift) for shift in fixed]
        fixed_other = [partner(value) for value in fixed_own]
        held = swapped_with_all(copies, "z")
        if extra is None:
            (held,) = small_call(pick_kernel, "pick", z_items, [held], [(moves, items, rank)])
            y_steps, x_steps = y_items, x_items
        else:
            units = moves * (items // users)
            shape = (units + moves, users, rank)
            (held,) = small_call(pick_items_kernel, "pick_items", z_items, [held, extra], [shape])
            y_steps = jnp.concatenate([jnp.repeat(y_items, items // users), y_marks])
            x_steps = jnp.concatenate([jnp.repeat(x_items, items // users), x_marks])
        held = stepped(stepped(held, "y", y_steps), "x", x_steps)
        if extra is not None:
            extra = held[units:]
            held = held[:units].reshape(moves, items, rank)
        return [*fixed_own, held], [*fixed_other, partner(held)], extra

    copies = jnp.broadcast_to(item_start, (nz, items, rank))
    own, other, moved = gather_items(item_start, copies, marks[len(fixed) :])
    held = solve_users(own, other, own_marks, other_marks, nz, moved)

    held = swapped_with_all(held, "z")
    copies, moved = small_call(
        pick_users_kernel, "pick_users", z_users, [held], [(nx * ny, tiles, rows, rank), (moves, users, items)]
    )
    held = swapped_with_all(copies, ("x", "y"))
    (own_users,) = small_call(pick_own_kernel, "pick_own", x_users * ny + y_users, [held], [(tiles, rows, rank)])
    item_factors, copies = solve_items(own_users, partner(own_users), [*fixed_marks, moved], nz)

    own, other, _ = gather_items(item_factors, copies, None)
    user_factors = solve_users(own, other, own_marks, other_marks)
    return (user_factors, item_factors)


def solution(mesh):
    torus = Mesh(mesh.devices.reshape(4, 4, 8, 2), (*AXES, "grp"))
    everywhere = (*AXES, "grp")
    in_specs = (P(everywhere, None), P(None, AXES, "grp"), P(None, AXES), P())
    out_specs = (P(everywhere, None), P(everywhere, None))
    return jax.shard_map(body, mesh=torus, in_specs=in_specs, out_specs=out_specs, check_vma=False)
```

```python
import functools

import jax
import jax.numpy as jnp
from jax import lax
from jax.experimental import pallas as pl
from jax.experimental.pallas import tpu as pltpu
from jax.sharding import Mesh, PartitionSpec as P

SWEEPS = 4
RIDGE = 0.005
UNRATED = 64.0
RATED_BELOW = 32.0
AXES = ("x", "y", "z")
VMEM = pltpu.MemorySpace.VMEM
SMEM = pltpu.MemorySpace.SMEM


def split_parts(value):
    high = value.astype(jnp.bfloat16)
    low = (value - high.astype(jnp.float32)).astype(jnp.bfloat16)
    return jnp.concatenate([high, low], axis=0)


def dot_f32(a, b, dims=((1,), (0,))):
    return lax.dot_general(a, b, (dims, ((), ())), preferred_element_type=jnp.float32)


def relax(right, ridge, bound, rated, factors):
    rows = right.shape[0]
    inverse = 1.0 / bound
    answer = right * inverse
    for _ in range(SWEEPS - 1):
        inner = dot_f32(split_parts(answer), factors, ((1,), (1,)))
        inner = jnp.where(rated, inner[:rows] + inner[rows:], 0.0)
        outer = dot_f32(split_parts(inner), factors)
        applied = outer[:rows] + outer[rows:] + ridge * answer
        answer = answer + (right - applied) * inverse
    return answer.astype(jnp.bfloat16)


def users_kernel(*refs, tiles, copies):
    own, other = refs[:tiles], refs[tiles : 2 * tiles]
    own_marks_ref, other_marks_ref, *extra, out_ref, factor_t_ref, mask_ref, sums_ref = refs[2 * tiles :]
    rank = own[0].shape[1]
    rows = own_marks_ref.shape[1]
    parts = []
    for k in range(tiles):
        parts += [own[k][...], other[k][...]]
    marks = []
    for k in range(own_marks_ref.shape[0]):
        marks += [own_marks_ref[k], other_marks_ref[k]]
    factors = jnp.concatenate(parts, axis=0)
    marked = jnp.concatenate(marks, axis=1).astype(jnp.float32)
    rated = jnp.abs(marked) < RATED_BELOW
    factor_t_ref[...] = factors.T
    mask = jnp.where(rated, 1.0, 0.0)
    mask_ref[...] = mask
    count = jnp.sum(mask, axis=1, keepdims=True)
    right = dot_f32(jnp.where(rated, marked, 0.0).astype(jnp.bfloat16), factors)
    together = 16

    def some(step, carry):
        chosen = mask_ref[pl.ds(step * together, together), :].astype(jnp.bfloat16)
        weighted = (factor_t_ref[...][None] * chosen[:, None, :]).reshape(together * rank, -1)
        gram = dot_f32(weighted, factors)
        total = jnp.sum(jnp.abs(gram).reshape(together, rank, rank), axis=1)
        sums_ref[pl.ds(step * together, together), :] = total
        return carry

    lax.fori_loop(0, rows // together, some, 0)
    ridge = RIDGE * (count + 1.0)
    bound = jnp.max(sums_ref[...], axis=1, keepdims=True) + ridge
    answer = relax(right, ridge, bound, rated, factors)
    if not copies:
        out_ref[...] = answer
    for c in range(copies):
        out_ref[c, :rows, :] = answer
        for k, ref in enumerate(extra):
            users = ref.shape[0]
            out_ref[c, rows + k * users : rows + (k + 1) * users, :] = ref[...]


def items_kernel(*refs):
    *ins, out_ref, copies_ref, sums_ref = refs
    own, other, marks = (ins[i * len(ins) // 3 : (i + 1) * len(ins) // 3] for i in range(3))
    rank = own[0].shape[1]
    items = out_ref.shape[0]
    parts = []
    for k in range(len(own)):
        parts += [own[k][...], other[k][...]]
    factors = jnp.concatenate(parts, axis=0)
    factor_t = factors.T
    marked = jnp.concatenate([ref[...].astype(jnp.float32) for ref in marks], axis=0).T
    rated = jnp.abs(marked) < RATED_BELOW
    mask = jnp.where(rated, 1.0, 0.0)
    count = jnp.sum(mask, axis=1, keepdims=True)
    right = dot_f32(jnp.where(rated, marked, 0.0).astype(jnp.bfloat16), factors)
    group = 8
    for j in range(items // group):
        row = mask[j * group : j * group + 1].astype(jnp.bfloat16)
        gram = dot_f32(factor_t * row, factors)
        total = jnp.sum(jnp.abs(gram), axis=0, keepdims=True)
        sums_ref[j * group : (j + 1) * group, :] = jnp.broadcast_to(total, (group, rank))
    ridge = RIDGE * (count + 1.0)
    bound = jnp.max(sums_ref[...], axis=1, keepdims=True) + ridge
    answer = relax(right, ridge, bound, rated, factors)
    out_ref[...] = answer
    for c in range(copies_ref.shape[0]):
        copies_ref[c] = answer


def vmem_specs(count):
    return [pl.BlockSpec(memory_space=VMEM)] * count


def solve_users(own, other, own_marks, other_marks, copies=0, extra=()):
    tiles, rows, half = own_marks.shape
    rank = own[0].shape[1]
    width = tiles * 2 * half
    args = [*own, *other, own_marks, other_marks, *extra]
    shape = (rows, rank)
    if copies:
        shape = (copies, rows + sum(e.shape[0] for e in extra), rank)
    return pl.pallas_call(
        functools.partial(users_kernel, tiles=tiles, copies=copies),
        out_shape=jax.ShapeDtypeStruct(shape, jnp.bfloat16),
        in_specs=vmem_specs(len(args)),
        out_specs=pl.BlockSpec(memory_space=VMEM),
        scratch_shapes=[
            pltpu.VMEM((rank, width), jnp.bfloat16),
            pltpu.VMEM((rows, width), jnp.float32),
            pltpu.VMEM((rows, rank), jnp.float32),
        ],
        name="users",
    )(*args)


def solve_items(own, other, marks, copies):
    rank = own[0].shape[1]
    items = marks[0].shape[1]
    args = [*own, *other, *marks]
    return pl.pallas_call(
        items_kernel,
        out_shape=(
            jax.ShapeDtypeStruct((items, rank), jnp.bfloat16),
            jax.ShapeDtypeStruct((copies, items, rank), jnp.bfloat16),
        ),
        in_specs=vmem_specs(len(args)),
        out_specs=tuple(vmem_specs(2)),
        scratch_shapes=[pltpu.VMEM((items, rank), jnp.float32)],
        name="items",
    )(*args)


def swapped_with_all(copies, axes):
    return lax.all_to_all(copies, axes, split_axis=0, concat_axis=0, tiled=True)


def fetched_from(value, axis, steps):
    count = 1
    for name in (axis if isinstance(axis, tuple) else (axis,)):
        count *= lax.axis_size(name)
    return lax.ppermute(value, axis, [((target + steps) % count, target) for target in range(count)])


def shift_digits(shift, z_first):
    nz, ny, nx = lax.axis_size("z"), lax.axis_size("y"), lax.axis_size("x")
    z, z_shift = lax.axis_index("z"), shift % nz
    carry = (z + z_shift) // nz if z_first else jnp.where(z < z_shift, 1, 0)
    y = lax.axis_index("y") + (shift // nz) % ny + carry
    x = lax.axis_index("x") + shift // (nz * ny) + y // ny
    return (x % nx) * ny + y % ny, (z + z_shift) % nz


def taken(source, index, start, size):
    picked = lax.dynamic_slice(source, (index, jnp.int32(start), jnp.int32(0)), (1, size, source.shape[2]))
    return picked[0]


def body(item_start, ratings, rating_bits, plan):
    tiles, users, items = ratings.shape
    own_half = lax.axis_index("grp")
    blocks = lax.axis_size(AXES)
    plane = lax.axis_size(("x", "y"))
    ring = lax.axis_size("z")
    rows = users // 2
    partner = lambda value: fetched_from(value, "grp", 1)

    near, across = blocks - 1, blocks // 2
    place = lambda wanted: jnp.sum(jnp.where(plan == wanted, jnp.arange(tiles), 0))
    first, second = place(near), place(across)
    low, high = jnp.minimum(first, second), jnp.maximum(first, second)
    third = jnp.where(low > 0, 0, jnp.where(high > 1, 1, 2))
    fourth = tiles * (tiles - 1) // 2 - first - second - third
    order = (first, second, third, fourth)
    shifts = (near, across, plan[third], plan[fourth])
    forward = [shift_digits(shift, False) for shift in shifts]
    backward = [shift_digits((blocks - shift) % blocks, False) for shift in shifts]
    marks_at = [shift_digits(blocks - shift, True) for shift in shifts[2:]]

    bit_count = 32 // lax.axis_size("grp")
    item_bits = own_half * bit_count + lax.broadcasted_iota(jnp.int32, (1, 1, items), 2) // (items // bit_count)
    rated = (jnp.right_shift(rating_bits[:, :, None], item_bits) & 1) == 1
    marks = jnp.where(rated, ratings, jnp.asarray(UNRATED, ratings.dtype))
    cut = lambda k, at: lax.dynamic_slice(marks, (k, at * rows, 0), (1, rows, items))[0]
    own_marks = [cut(k, own_half) for k in order]
    away_marks = [cut(k, 1 - own_half) for k in order]
    marks = [jnp.concatenate(pair, axis=0) for pair in zip(own_marks, away_marks)]
    own_marks = jnp.stack(own_marks)
    other_marks = partner(jnp.stack(away_marks))

    def gather(copies, size, digits, z_step, extra=()):
        held = swapped_with_all(copies, ("x", "y"))
        pieces = [taken(held, at, 0, size) for at, _ in digits]
        pieces[0] = fetched_from(pieces[0], "z", z_step)
        moving = jnp.concatenate([*pieces[2:], *extra], axis=0)
        ring_held = swapped_with_all(jnp.broadcast_to(moving, (ring, *moving.shape)), "z")
        for k in (2, 3):
            pieces[k] = taken(ring_held, digits[k][1], (k - 2) * size, size)
        return held, ring_held, pieces, [partner(piece) for piece in pieces]

    copies = jnp.broadcast_to(item_start, (plane, *item_start.shape))
    _, held, own, other = gather(copies, items, forward, -1, marks[2:])
    moved = [taken(held, z_at, 2 * items + k * users, users) for k, (_, z_at) in enumerate(marks_at)]
    near_marks, across_marks = (fetched_from(m, AXES, -shift) for m, shift in zip(marks, (near, across)))
    near_marks, across_marks, *moved = lax.optimization_barrier((near_marks, across_marks, *moved))
    copies = solve_users(own, other, own_marks, other_marks, plane, moved)

    held, _, own, other = gather(copies, rows, backward, 1)
    moved = [taken(held, at, rows + k * users, users) for k, (at, _) in enumerate(marks_at)]
    item_factors, copies = solve_items(own, other, [near_marks, across_marks, *moved], plane)

    _, _, own, other = gather(copies, items, forward, -1)
    user_factors = solve_users(own, other, own_marks, other_marks)
    return (user_factors, item_factors)


def solution(mesh):
    torus = Mesh(mesh.devices.reshape(4, 4, 8, 2), (*AXES, "grp"))
    everywhere = (*AXES, "grp")
    in_specs = (P(everywhere, None), P(None, AXES, "grp"), P(None, AXES), P())
    out_specs = (P(everywhere, None), P(everywhere, None))
    return jax.shard_map(body, mesh=torus, in_specs=in_specs, out_specs=out_specs, check_vma=False)
```

```python
import functools

import jax
import jax.numpy as jnp
from jax import lax
from jax.experimental import pallas as pl
from jax.experimental.pallas import tpu as pltpu
from jax.sharding import Mesh, PartitionSpec as P

SWEEPS = 4
RIDGE = 0.005
UNRATED = 64.0
RATED_BELOW = 32.0
AXES = ("x", "y", "z")
VMEM = pltpu.MemorySpace.VMEM
SMEM = pltpu.MemorySpace.SMEM


def split_parts(value):
    high = value.astype(jnp.bfloat16)
    low = (value - high.astype(jnp.float32)).astype(jnp.bfloat16)
    return jnp.concatenate([high, low], axis=0)


def dot_f32(a, b, dims=((1,), (0,))):
    return lax.dot_general(a, b, (dims, ((), ())), preferred_element_type=jnp.float32)


def relax(right, ridge, bound, rated, factors):
    rows = right.shape[0]
    inverse = 1.0 / bound
    answer = right * inverse
    for _ in range(SWEEPS - 1):
        inner = dot_f32(split_parts(answer), factors, ((1,), (1,)))
        inner = jnp.where(rated, inner[:rows] + inner[rows:], 0.0)
        outer = dot_f32(split_parts(inner), factors)
        applied = outer[:rows] + outer[rows:] + ridge * answer
        answer = answer + (right - applied) * inverse
    return answer.astype(jnp.bfloat16)


def users_kernel(*refs, tiles, copies):
    own, other = refs[:tiles], refs[tiles : 2 * tiles]
    own_marks_ref, other_marks_ref, *rest, factor_t_ref, mask_ref, sums_ref = refs[2 * tiles :]
    copies_ref = rest.pop() if copies else None
    *extra, out_ref = rest
    rank = own[0].shape[1]
    rows = own_marks_ref.shape[1]
    parts = []
    for k in range(tiles):
        parts += [own[k][...], other[k][...]]
    marks = []
    for k in range(own_marks_ref.shape[0]):
        marks += [own_marks_ref[k], other_marks_ref[k]]
    factors = jnp.concatenate(parts, axis=0)
    marked = jnp.concatenate(marks, axis=1).astype(jnp.float32)
    rated = jnp.abs(marked) < RATED_BELOW
    factor_t_ref[...] = factors.T
    mask = jnp.where(rated, 1.0, 0.0)
    mask_ref[...] = mask
    count = jnp.sum(mask, axis=1, keepdims=True)
    right = dot_f32(jnp.where(rated, marked, 0.0).astype(jnp.bfloat16), factors)
    together = 16

    def some(step, carry):
        chosen = mask_ref[pl.ds(step * together, together), :].astype(jnp.bfloat16)
        weighted = (factor_t_ref[...][None] * chosen[:, None, :]).reshape(together * rank, -1)
        gram = dot_f32(weighted, factors)
        total = jnp.sum(jnp.abs(gram).reshape(together, rank, rank), axis=1)
        sums_ref[pl.ds(step * together, together), :] = total
        return carry

    lax.fori_loop(0, rows // together, some, 0)
    ridge = RIDGE * (count + 1.0)
    bound = jnp.max(sums_ref[...], axis=1, keepdims=True) + ridge
    answer = relax(right, ridge, bound, rated, factors)
    out_ref[...] = answer
    for c in range(copies):
        copies_ref[c, :rows, :] = answer
        for k, ref in enumerate(extra):
            users = ref.shape[0]
            copies_ref[c, rows + k * users : rows + (k + 1) * users, :] = ref[...]


def items_kernel(*refs):
    *ins, out_ref, copies_ref, sums_ref = refs
    own, other, marks = (ins[i * len(ins) // 3 : (i + 1) * len(ins) // 3] for i in range(3))
    rank = own[0].shape[1]
    items = out_ref.shape[0]
    parts = []
    for k in range(len(own)):
        parts += [own[k][...], other[k][...]]
    factors = jnp.concatenate(parts, axis=0)
    factor_t = factors.T
    marked = jnp.concatenate([ref[...].astype(jnp.float32) for ref in marks], axis=0).T
    rated = jnp.abs(marked) < RATED_BELOW
    mask = jnp.where(rated, 1.0, 0.0)
    count = jnp.sum(mask, axis=1, keepdims=True)
    right = dot_f32(jnp.where(rated, marked, 0.0).astype(jnp.bfloat16), factors)
    group = 8
    kinds = items // group
    chosen = jnp.concatenate([mask[j * group : j * group + 1] for j in range(kinds)], axis=0).astype(jnp.bfloat16)
    weighted = (factor_t[None] * chosen[:, None, :]).reshape(kinds * rank, -1)
    gram = dot_f32(weighted, factors)
    total = jnp.sum(jnp.abs(gram).reshape(kinds, rank, rank), axis=1)
    for j in range(kinds):
        sums_ref[j * group : (j + 1) * group, :] = jnp.broadcast_to(total[j : j + 1], (group, rank))
    ridge = RIDGE * (count + 1.0)
    bound = jnp.max(sums_ref[...], axis=1, keepdims=True) + ridge
    answer = relax(right, ridge, bound, rated, factors)
    out_ref[...] = answer
    for c in range(copies_ref.shape[0]):
        copies_ref[c] = answer


def vmem_specs(count):
    return [pl.BlockSpec(memory_space=VMEM)] * count


def solve_users(own, other, own_marks, other_marks, copies=0, extra=()):
    tiles, rows, half = own_marks.shape
    rank = own[0].shape[1]
    width = tiles * 2 * half
    args = [*own, *other, own_marks, other_marks, *extra]
    shapes = [(rows, rank)]
    if copies:
        shapes.append((copies, rows + sum(e.shape[0] for e in extra), rank))
    return pl.pallas_call(
        functools.partial(users_kernel, tiles=tiles, copies=copies),
        out_shape=tuple(jax.ShapeDtypeStruct(shape, jnp.bfloat16) for shape in shapes),
        in_specs=vmem_specs(len(args)),
        out_specs=tuple(vmem_specs(len(shapes))),
        scratch_shapes=[
            pltpu.VMEM((rank, width), jnp.bfloat16),
            pltpu.VMEM((rows, width), jnp.float32),
            pltpu.VMEM((rows, rank), jnp.float32),
        ],
        name="users",
    )(*args)


def solve_items(own, other, marks, copies):
    rank = own[0].shape[1]
    items = marks[0].shape[1]
    args = [*own, *other, *marks]
    return pl.pallas_call(
        items_kernel,
        out_shape=(
            jax.ShapeDtypeStruct((items, rank), jnp.bfloat16),
            jax.ShapeDtypeStruct((copies, items, rank), jnp.bfloat16),
        ),
        in_specs=vmem_specs(len(args)),
        out_specs=tuple(vmem_specs(2)),
        scratch_shapes=[pltpu.VMEM((items, rank), jnp.float32)],
        name="items",
    )(*args)


def swapped_with_all(copies, axes):
    return lax.all_to_all(copies, axes, split_axis=0, concat_axis=0, tiled=True)


def fetched_from(value, axis, steps):
    count = 1
    for name in (axis if isinstance(axis, tuple) else (axis,)):
        count *= lax.axis_size(name)
    return lax.ppermute(value, axis, [((target + steps) % count, target) for target in range(count)])


def place_on(axis):
    return lax.axis_index(axis).astype(jnp.uint32)


def shift_digits(shift, z_first):
    ring, plane = lax.axis_size("z"), lax.axis_size(("x", "y"))
    z_bits = ring.bit_length() - 1
    z, z_shift = place_on("z"), shift & (ring - 1)
    carry = (z + z_shift) >> z_bits if z_first else (z < z_shift).astype(jnp.uint32)
    return (place_on(("x", "y")) + (shift >> z_bits) + carry) & (plane - 1), (z + z_shift) & (ring - 1)


def taken(source, index, start, size):
    zero = jnp.uint32(0)
    return lax.dynamic_slice(source, (index, zero + start, zero), (1, size, source.shape[2]))[0]


def body(item_start, ratings, rating_bits, plan):
    tiles, users, items = ratings.shape
    own_half = lax.axis_index("grp")
    blocks = lax.axis_size(AXES)
    plane = lax.axis_size(("x", "y"))
    ring = lax.axis_size("z")
    rows = users // 2
    partner = lambda value: fetched_from(value, "grp", 1)

    near, across = blocks - 1, blocks // 2
    offsets = [plan[k].astype(jnp.uint32) for k in range(tiles)]
    zero = jnp.uint32(0)

    def place(wanted):
        at = zero
        for k in range(1, tiles):
            at = jnp.where(offsets[k] == wanted, jnp.uint32(k), at)
        return at

    first, second = place(near), place(across)
    low, high = jnp.minimum(first, second), jnp.maximum(first, second)
    third = jnp.where(low > 0, zero, jnp.where(high > 1, jnp.uint32(1), jnp.uint32(2)))
    fourth = jnp.uint32(tiles * (tiles - 1) // 2) - first - second - third
    order = (first, second, third, fourth)

    def offset_at(k):
        value = offsets[0]
        for j in range(1, tiles):
            value = jnp.where(k == j, offsets[j], value)
        return value

    shifts = (jnp.uint32(near), jnp.uint32(across), offset_at(third), offset_at(fourth))
    forward = [shift_digits(shift, False) for shift in shifts]
    backward = [shift_digits(blocks - shift, False) for shift in shifts]
    marks_at = [shift_digits(blocks - shift, True) for shift in shifts[2:]]

    bit_count = 32 // lax.axis_size("grp")
    item_bits = own_half * bit_count + lax.broadcasted_iota(jnp.int32, (1, 1, items), 2) // (items // bit_count)
    rated = (jnp.right_shift(rating_bits[:, :, None], item_bits) & 1) == 1
    marks = jnp.where(rated, ratings, jnp.asarray(UNRATED, ratings.dtype))
    own_row = place_on("grp") * rows
    cut = lambda k, at: lax.dynamic_slice(marks, (k, at, zero), (1, rows, items))[0]
    own_marks = [cut(k, own_row) for k in order]
    away_marks = [cut(k, rows - own_row) for k in order]
    marks = [jnp.concatenate(pair, axis=0) for pair in zip(own_marks, away_marks)]
    own_marks = jnp.stack(own_marks)
    other_marks = partner(jnp.stack(away_marks))

    def gather(shard, copies, digits, near_shift, extra=()):
        size = shard.shape[0]
        neighbour = fetched_from(shard, AXES, near_shift)
        held = swapped_with_all(copies, ("x", "y"))
        pieces = [neighbour] + [taken(held, at, 0, size) for at, _ in digits[1:]]
        moving = jnp.concatenate([*pieces[2:], *extra], axis=0)
        ring_held = swapped_with_all(jnp.broadcast_to(moving, (ring, *moving.shape)), "z")
        for k in (2, 3):
            pieces[k] = taken(ring_held, digits[k][1], (k - 2) * size, size)
        return held, ring_held, pieces, [partner(piece) for piece in pieces]

    copies = jnp.broadcast_to(item_start, (plane, *item_start.shape))
    _, held, own, other = gather(item_start, copies, forward, near, marks[2:])
    moved = [taken(held, z_at, 2 * items + k * users, users) for k, (_, z_at) in enumerate(marks_at)]
    near_marks, across_marks = (fetched_from(m, AXES, -shift) for m, shift in zip(marks, (near, across)))
    near_marks, across_marks, *moved = lax.optimization_barrier((near_marks, across_marks, *moved))
    first_users, copies = solve_users(own, other, own_marks, other_marks, plane, moved)

    held, _, own, other = gather(first_users, copies, backward, -near)
    moved = [taken(held, at, rows + k * users, users) for k, (at, _) in enumerate(marks_at)]
    item_factors, copies = solve_items(own, other, [near_marks, across_marks, *moved], plane)

    _, _, own, other = gather(item_factors, copies, forward, near)
    (user_factors,) = solve_users(own, other, own_marks, other_marks)
    return (user_factors, item_factors)


def solution(mesh):
    torus = Mesh(mesh.devices.reshape(4, 4, 8, 2), (*AXES, "grp"))
    everywhere = (*AXES, "grp")
    in_specs = (P(everywhere, None), P(None, AXES, "grp"), P(None, AXES), P())
    out_specs = (P(everywhere, None), P(everywhere, None))
    return jax.shard_map(body, mesh=torus, in_specs=in_specs, out_specs=out_specs, check_vma=False)
```

```python
import functools

import jax
import jax.numpy as jnp
from jax import lax
from jax.experimental import pallas as pl
from jax.experimental.pallas import tpu as pltpu
from jax.sharding import Mesh, PartitionSpec as P

SWEEPS = 4
RIDGE = 0.005
UNRATED = 64.0
RATED_BELOW = 32.0
AXES = ("x", "y", "z")
VMEM = pltpu.MemorySpace.VMEM
SMEM = pltpu.MemorySpace.SMEM


def split_parts(value):
    high = value.astype(jnp.bfloat16)
    low = (value - high.astype(jnp.float32)).astype(jnp.bfloat16)
    return jnp.concatenate([high, low], axis=0)


def dot_f32(a, b, dims=((1,), (0,))):
    return lax.dot_general(a, b, (dims, ((), ())), preferred_element_type=jnp.float32)


def relax(right, ridge, bound, rated, factors):
    rows = right.shape[0]
    inverse = 1.0 / bound
    answer = right * inverse
    for _ in range(SWEEPS - 1):
        inner = dot_f32(split_parts(answer), factors, ((1,), (1,)))
        inner = jnp.where(rated, inner[:rows] + inner[rows:], 0.0)
        outer = dot_f32(split_parts(inner), factors)
        applied = outer[:rows] + outer[rows:] + ridge * answer
        answer = answer + (right - applied) * inverse
    return answer.astype(jnp.bfloat16)


def users_kernel(*refs, tiles, copies):
    own, other = refs[:tiles], refs[tiles : 2 * tiles]
    own_marks_ref, other_marks_ref, *rest, factor_t_ref, mask_ref, sums_ref = refs[2 * tiles :]
    copies_ref = rest.pop() if copies else None
    *extra, out_ref = rest
    rank = own[0].shape[1]
    rows = own_marks_ref.shape[1]
    parts = []
    for k in range(tiles):
        parts += [own[k][...], other[k][...]]
    marks = []
    for k in range(own_marks_ref.shape[0]):
        marks += [own_marks_ref[k], other_marks_ref[k]]
    factors = jnp.concatenate(parts, axis=0)
    marked = jnp.concatenate(marks, axis=1).astype(jnp.float32)
    rated = jnp.abs(marked) < RATED_BELOW
    factor_t_ref[...] = factors.T
    mask = jnp.where(rated, 1.0, 0.0)
    mask_ref[...] = mask
    count = jnp.sum(mask, axis=1, keepdims=True)
    right = dot_f32(jnp.where(rated, marked, 0.0).astype(jnp.bfloat16), factors)
    together = 16

    def some(step, carry):
        chosen = mask_ref[pl.ds(step * together, together), :].astype(jnp.bfloat16)
        weighted = (factor_t_ref[...][None] * chosen[:, None, :]).reshape(together * rank, -1)
        gram = dot_f32(weighted, factors)
        total = jnp.sum(jnp.abs(gram).reshape(together, rank, rank), axis=1)
        sums_ref[pl.ds(step * together, together), :] = total
        return carry

    lax.fori_loop(0, rows // together, some, 0)
    ridge = RIDGE * (count + 1.0)
    bound = jnp.max(sums_ref[...], axis=1, keepdims=True) + ridge
    answer = relax(right, ridge, bound, rated, factors)
    out_ref[...] = answer
    for c in range(copies):
        copies_ref[c, :rows, :] = answer
        for k, ref in enumerate(extra):
            users = ref.shape[0]
            copies_ref[c, rows + k * users : rows + (k + 1) * users, :] = ref[...]


def items_kernel(*refs):
    *ins, out_ref, copies_ref, sums_ref = refs
    own, other, marks = (ins[i * len(ins) // 3 : (i + 1) * len(ins) // 3] for i in range(3))
    rank = own[0].shape[1]
    items = out_ref.shape[0]
    parts = []
    for k in range(len(own)):
        parts += [own[k][...], other[k][...]]
    factors = jnp.concatenate(parts, axis=0)
    factor_t = factors.T
    marked = jnp.concatenate([ref[...].astype(jnp.float32) for ref in marks], axis=0).T
    rated = jnp.abs(marked) < RATED_BELOW
    mask = jnp.where(rated, 1.0, 0.0)
    count = jnp.sum(mask, axis=1, keepdims=True)
    right = dot_f32(jnp.where(rated, marked, 0.0).astype(jnp.bfloat16), factors)
    group = 8
    for j in range(items // group):
        row = mask[j * group : j * group + 1].astype(jnp.bfloat16)
        gram = dot_f32(factor_t * row, factors)
        total = jnp.sum(jnp.abs(gram), axis=0, keepdims=True)
        sums_ref[j * group : (j + 1) * group, :] = jnp.broadcast_to(total, (group, rank))
    ridge = RIDGE * (count + 1.0)
    bound = jnp.max(sums_ref[...], axis=1, keepdims=True) + ridge
    answer = relax(right, ridge, bound, rated, factors)
    out_ref[...] = answer
    for c in range(copies_ref.shape[0]):
        copies_ref[c] = answer


def vmem_specs(count):
    return [pl.BlockSpec(memory_space=VMEM)] * count


def solve_users(own, other, own_marks, other_marks, copies=0, extra=()):
    tiles, rows, half = own_marks.shape
    rank = own[0].shape[1]
    width = tiles * 2 * half
    args = [*own, *other, own_marks, other_marks, *extra]
    shapes = [(rows, rank)]
    if copies:
        shapes.append((copies, rows + sum(e.shape[0] for e in extra), rank))
    return pl.pallas_call(
        functools.partial(users_kernel, tiles=tiles, copies=copies),
        out_shape=tuple(jax.ShapeDtypeStruct(shape, jnp.bfloat16) for shape in shapes),
        in_specs=vmem_specs(len(args)),
        out_specs=tuple(vmem_specs(len(shapes))),
        scratch_shapes=[
            pltpu.VMEM((rank, width), jnp.bfloat16),
            pltpu.VMEM((rows, width), jnp.float32),
            pltpu.VMEM((rows, rank), jnp.float32),
        ],
        name="users",
    )(*args)


def solve_items(own, other, marks, copies):
    rank = own[0].shape[1]
    items = marks[0].shape[1]
    args = [*own, *other, *marks]
    return pl.pallas_call(
        items_kernel,
        out_shape=(
            jax.ShapeDtypeStruct((items, rank), jnp.bfloat16),
            jax.ShapeDtypeStruct((copies, items, rank), jnp.bfloat16),
        ),
        in_specs=vmem_specs(len(args)),
        out_specs=tuple(vmem_specs(2)),
        scratch_shapes=[pltpu.VMEM((items, rank), jnp.float32)],
        name="items",
    )(*args)


def swapped_with_all(copies, axes):
    return lax.all_to_all(copies, axes, split_axis=0, concat_axis=0, tiled=True)


def fetched_from(value, axis, steps):
    count = 1
    for name in (axis if isinstance(axis, tuple) else (axis,)):
        count *= lax.axis_size(name)
    return lax.ppermute(value, axis, [((target + steps) % count, target) for target in range(count)])


def place_on(axis):
    return lax.axis_index(axis).astype(jnp.uint32)


def shift_digits(shift, z_first):
    ring, plane = lax.axis_size("z"), lax.axis_size(("x", "y"))
    z_bits = ring.bit_length() - 1
    z, z_shift = place_on("z"), shift & (ring - 1)
    carry = (z + z_shift) >> z_bits if z_first else (z < z_shift).astype(jnp.uint32)
    return (place_on(("x", "y")) + (shift >> z_bits) + carry) & (plane - 1), (z + z_shift) & (ring - 1)


def taken(source, index, start, size):
    zero = jnp.uint32(0)
    return lax.dynamic_slice(source, (index, zero + start, zero), (1, size, source.shape[2]))[0]


def body(item_start, ratings, rating_bits, plan):
    tiles, users, items = ratings.shape
    own_half = lax.axis_index("grp")
    blocks = lax.axis_size(AXES)
    plane = lax.axis_size(("x", "y"))
    ring = lax.axis_size("z")
    rows = users // 2
    partner = lambda value: fetched_from(value, "grp", 1)

    near, across = blocks - 1, blocks // 2
    offsets = [plan[k].astype(jnp.uint32) for k in range(tiles)]
    zero = jnp.uint32(0)

    def place(wanted):
        at = zero
        for k in range(1, tiles):
            at = jnp.where(offsets[k] == wanted, jnp.uint32(k), at)
        return at

    first, second = place(near), place(across)
    low, high = jnp.minimum(first, second), jnp.maximum(first, second)
    third = jnp.where(low > 0, zero, jnp.where(high > 1, jnp.uint32(1), jnp.uint32(2)))
    fourth = jnp.uint32(tiles * (tiles - 1) // 2) - first - second - third
    order = (first, second, third, fourth)

    def offset_at(k):
        value = offsets[0]
        for j in range(1, tiles):
            value = jnp.where(k == j, offsets[j], value)
        return value

    shifts = (jnp.uint32(near), jnp.uint32(across), offset_at(third), offset_at(fourth))
    forward = [shift_digits(shift, False) for shift in shifts]
    backward = [shift_digits(blocks - shift, False) for shift in shifts]
    marks_at = [shift_digits(blocks - shift, True) for shift in shifts[2:]]

    bit_count = 32 // lax.axis_size("grp")
    item_bits = own_half * bit_count + lax.broadcasted_iota(jnp.int32, (1, 1, items), 2) // (items // bit_count)
    rated = (jnp.right_shift(rating_bits[:, :, None], item_bits) & 1) == 1
    marks = jnp.where(rated, ratings, jnp.asarray(UNRATED, ratings.dtype))
    own_row = place_on("grp") * rows
    cut = lambda k, at: lax.dynamic_slice(marks, (k, at, zero), (1, rows, items))[0]
    own_marks = [cut(k, own_row) for k in order]
    away_marks = [cut(k, rows - own_row) for k in order]
    marks = [jnp.concatenate(pair, axis=0) for pair in zip(own_marks, away_marks)]
    own_marks = jnp.stack(own_marks)
    other_marks = partner(jnp.stack(away_marks))

    def gather(shard, copies, digits, near_shift, extra=(), direct=()):
        size = shard.shape[0]
        neighbour = fetched_from(shard, AXES, near_shift)
        held = swapped_with_all(copies, ("x", "y"))
        pieces = [neighbour] + [taken(held, at, 0, size) for at, _ in digits[1:]]
        moving = jnp.concatenate([*pieces[2:], *extra], axis=0)
        moving, pieces[0], *direct = lax.optimization_barrier((moving, neighbour, *direct))
        ring_held = swapped_with_all(jnp.broadcast_to(moving, (ring, *moving.shape)), "z")
        for k in (2, 3):
            pieces[k] = taken(ring_held, digits[k][1], (k - 2) * size, size)
        return held, ring_held, pieces, [partner(piece) for piece in pieces], direct

    copies = jnp.broadcast_to(item_start, (plane, *item_start.shape))
    sent = [fetched_from(m, AXES, -shift) for m, shift in zip(marks, (near, across))]
    _, held, own, other, direct_marks = gather(item_start, copies, forward, near, marks[2:], sent)
    moved = [taken(held, z_at, 2 * items + k * users, users) for k, (_, z_at) in enumerate(marks_at)]
    first_users, copies = solve_users(own, other, own_marks, other_marks, plane, moved)

    held, _, own, other, _ = gather(first_users, copies, backward, -near)
    moved = [taken(held, at, rows + k * users, users) for k, (at, _) in enumerate(marks_at)]
    item_factors, copies = solve_items(own, other, [*direct_marks, *moved], plane)

    _, _, own, other, _ = gather(item_factors, copies, forward, near)
    (user_factors,) = solve_users(own, other, own_marks, other_marks)
    return (user_factors, item_factors)


def solution(mesh):
    torus = Mesh(mesh.devices.reshape(4, 4, 8, 2), (*AXES, "grp"))
    everywhere = (*AXES, "grp")
    in_specs = (P(everywhere, None), P(None, AXES, "grp"), P(None, AXES), P())
    out_specs = (P(everywhere, None), P(everywhere, None))
    return jax.shard_map(body, mesh=torus, in_specs=in_specs, out_specs=out_specs, check_vma=False)
```

```python
import functools

import jax
import jax.numpy as jnp
from jax import lax
from jax.experimental import pallas as pl
from jax.experimental.pallas import tpu as pltpu
from jax.sharding import Mesh, PartitionSpec as P

SWEEPS = 4
RIDGE = 0.005
UNRATED = 64.0
RATED_BELOW = 32.0
AXES = ("x", "y", "z")
VMEM = pltpu.MemorySpace.VMEM
SMEM = pltpu.MemorySpace.SMEM


def split_parts(value):
    high = value.astype(jnp.bfloat16)
    low = (value - high.astype(jnp.float32)).astype(jnp.bfloat16)
    return jnp.concatenate([high, low], axis=0)


def dot_f32(a, b, dims=((1,), (0,))):
    return lax.dot_general(a, b, (dims, ((), ())), preferred_element_type=jnp.float32)


def relax(right, ridge, bound, rated, factors):
    rows = right.shape[0]
    inverse = 1.0 / bound
    answer = right * inverse
    for _ in range(SWEEPS - 1):
        inner = dot_f32(split_parts(answer), factors, ((1,), (1,)))
        inner = jnp.where(rated, inner[:rows] + inner[rows:], 0.0)
        outer = dot_f32(split_parts(inner), factors)
        applied = outer[:rows] + outer[rows:] + ridge * answer
        answer = answer + (right - applied) * inverse
    return answer.astype(jnp.bfloat16)


def users_kernel(*refs, tiles, copies):
    own, other = refs[:tiles], refs[tiles : 2 * tiles]
    own_marks_ref, other_marks_ref, *rest, factor_t_ref, mask_ref, sums_ref = refs[2 * tiles :]
    copies_ref = rest.pop() if copies else None
    (out_ref,) = rest
    rank = own[0].shape[1]
    rows = own_marks_ref.shape[1]
    parts = []
    for k in range(tiles):
        parts += [own[k][...], other[k][...]]
    marks = []
    for k in range(own_marks_ref.shape[0]):
        marks += [own_marks_ref[k], other_marks_ref[k]]
    factors = jnp.concatenate(parts, axis=0)
    marked = jnp.concatenate(marks, axis=1).astype(jnp.float32)
    rated = jnp.abs(marked) < RATED_BELOW
    factor_t_ref[...] = factors.T
    mask = jnp.where(rated, 1.0, 0.0)
    mask_ref[...] = mask
    count = jnp.sum(mask, axis=1, keepdims=True)
    right = dot_f32(jnp.where(rated, marked, 0.0).astype(jnp.bfloat16), factors)
    together = 16

    def some(step, carry):
        chosen = mask_ref[pl.ds(step * together, together), :].astype(jnp.bfloat16)
        weighted = (factor_t_ref[...][None] * chosen[:, None, :]).reshape(together * rank, -1)
        gram = dot_f32(weighted, factors)
        total = jnp.sum(jnp.abs(gram).reshape(together, rank, rank), axis=1)
        sums_ref[pl.ds(step * together, together), :] = total
        return carry

    lax.fori_loop(0, rows // together, some, 0)
    ridge = RIDGE * (count + 1.0)
    bound = jnp.max(sums_ref[...], axis=1, keepdims=True) + ridge
    answer = relax(right, ridge, bound, rated, factors)
    out_ref[...] = answer
    for c in range(copies):
        copies_ref[c] = answer


def items_kernel(*refs):
    *ins, out_ref, copies_ref, sums_ref = refs
    own, other, marks = (ins[i * len(ins) // 3 : (i + 1) * len(ins) // 3] for i in range(3))
    rank = own[0].shape[1]
    items = out_ref.shape[0]
    parts = []
    for k in range(len(own)):
        parts += [own[k][...], other[k][...]]
    factors = jnp.concatenate(parts, axis=0)
    factor_t = factors.T
    marked = jnp.concatenate([ref[...].astype(jnp.float32) for ref in marks], axis=0).T
    rated = jnp.abs(marked) < RATED_BELOW
    mask = jnp.where(rated, 1.0, 0.0)
    count = jnp.sum(mask, axis=1, keepdims=True)
    right = dot_f32(jnp.where(rated, marked, 0.0).astype(jnp.bfloat16), factors)
    group = 8
    for j in range(items // group):
        row = mask[j * group : j * group + 1].astype(jnp.bfloat16)
        gram = dot_f32(factor_t * row, factors)
        total = jnp.sum(jnp.abs(gram), axis=0, keepdims=True)
        sums_ref[j * group : (j + 1) * group, :] = jnp.broadcast_to(total, (group, rank))
    ridge = RIDGE * (count + 1.0)
    bound = jnp.max(sums_ref[...], axis=1, keepdims=True) + ridge
    answer = relax(right, ridge, bound, rated, factors)
    out_ref[...] = answer
    for c in range(copies_ref.shape[0]):
        copies_ref[c] = answer


def vmem_specs(count):
    return [pl.BlockSpec(memory_space=VMEM)] * count


def solve_users(own, other, own_marks, other_marks, copies=0):
    tiles, rows, half = own_marks.shape
    rank = own[0].shape[1]
    width = tiles * 2 * half
    args = [*own, *other, own_marks, other_marks]
    shapes = [(rows, rank)]
    if copies:
        shapes.append((copies, rows, rank))
    return pl.pallas_call(
        functools.partial(users_kernel, tiles=tiles, copies=copies),
        out_shape=tuple(jax.ShapeDtypeStruct(shape, jnp.bfloat16) for shape in shapes),
        in_specs=vmem_specs(len(args)),
        out_specs=tuple(vmem_specs(len(shapes))),
        scratch_shapes=[
            pltpu.VMEM((rank, width), jnp.bfloat16),
            pltpu.VMEM((rows, width), jnp.float32),
            pltpu.VMEM((rows, rank), jnp.float32),
        ],
        name="users",
    )(*args)


def solve_items(own, other, marks, copies):
    rank = own[0].shape[1]
    items = marks[0].shape[1]
    args = [*own, *other, *marks]
    return pl.pallas_call(
        items_kernel,
        out_shape=(
            jax.ShapeDtypeStruct((items, rank), jnp.bfloat16),
            jax.ShapeDtypeStruct((copies, items, rank), jnp.bfloat16),
        ),
        in_specs=vmem_specs(len(args)),
        out_specs=tuple(vmem_specs(2)),
        scratch_shapes=[pltpu.VMEM((items, rank), jnp.float32)],
        name="items",
    )(*args)


def swapped_with_all(copies, axes):
    return lax.all_to_all(copies, axes, split_axis=0, concat_axis=0, tiled=True)


def fetched_from(value, axis, steps):
    count = 1
    for name in (axis if isinstance(axis, tuple) else (axis,)):
        count *= lax.axis_size(name)
    return lax.ppermute(value, axis, [((target + steps) % count, target) for target in range(count)])


def place_on(axis):
    return lax.axis_index(axis).astype(jnp.uint32)


def shift_digits(shift, z_first):
    ring, plane = lax.axis_size("z"), lax.axis_size(("x", "y"))
    z_bits = ring.bit_length() - 1
    z, z_shift = place_on("z"), shift & (ring - 1)
    carry = (z + z_shift) >> z_bits if z_first else (z < z_shift).astype(jnp.uint32)
    return (place_on(("x", "y")) + (shift >> z_bits) + carry) & (plane - 1), (z + z_shift) & (ring - 1)


def steps_to(place):
    ny, nx = lax.axis_size("y"), lax.axis_size("x")
    y, x = place & (ny - 1), place >> (ny.bit_length() - 1)
    return (y - place_on("y")) & (ny - 1), (x - place_on("x")) & (nx - 1)


def stepped(parts, axis, steps):
    held = jnp.concatenate(parts, axis=0)
    arrived = [held] + [fetched_from(held, axis, step) for step in range(1, lax.axis_size(axis))]
    chosen, start = [], 0
    for part, own_step in zip(parts, steps):
        value = part
        for step in range(1, len(arrived)):
            value = jnp.where(own_step == step, arrived[step][start : start + part.shape[0]], value)
        chosen.append(value)
        start += part.shape[0]
    return chosen


def taken(source, index, start, size):
    zero = jnp.uint32(0)
    return lax.dynamic_slice(source, (index, zero + start, zero), (1, size, source.shape[2]))[0]


def body(item_start, ratings, rating_bits, plan):
    tiles, users, items = ratings.shape
    own_half = lax.axis_index("grp")
    blocks = lax.axis_size(AXES)
    plane = lax.axis_size(("x", "y"))
    ring = lax.axis_size("z")
    rows = users // 2
    partner = lambda value: fetched_from(value, "grp", 1)

    near, across = blocks - 1, blocks // 2
    offsets = [plan[k].astype(jnp.uint32) for k in range(tiles)]
    zero = jnp.uint32(0)

    def place(wanted):
        at = zero
        for k in range(1, tiles):
            at = jnp.where(offsets[k] == wanted, jnp.uint32(k), at)
        return at

    first, second = place(near), place(across)
    low, high = jnp.minimum(first, second), jnp.maximum(first, second)
    third = jnp.where(low > 0, zero, jnp.where(high > 1, jnp.uint32(1), jnp.uint32(2)))
    fourth = jnp.uint32(tiles * (tiles - 1) // 2) - first - second - third
    order = (first, second, third, fourth)

    def offset_at(k):
        value = offsets[0]
        for j in range(1, tiles):
            value = jnp.where(k == j, offsets[j], value)
        return value

    shifts = (jnp.uint32(near), jnp.uint32(across), offset_at(third), offset_at(fourth))
    forward = [shift_digits(shift, True) for shift in shifts]
    backward = [shift_digits(blocks - shift, False) for shift in shifts]

    bit_count = 32 // lax.axis_size("grp")
    item_bits = own_half * bit_count + lax.broadcasted_iota(jnp.int32, (1, 1, items), 2) // (items // bit_count)
    rated = (jnp.right_shift(rating_bits[:, :, None], item_bits) & 1) == 1
    marks = jnp.where(rated, ratings, jnp.asarray(UNRATED, ratings.dtype))
    own_row = place_on("grp") * rows
    cut = lambda k, at: lax.dynamic_slice(marks, (k, at, zero), (1, rows, items))[0]
    own_marks = [cut(k, own_row) for k in order]
    away_marks = [cut(k, rows - own_row) for k in order]
    marks = [jnp.concatenate(pair, axis=0) for pair in zip(own_marks, away_marks)]
    own_marks = jnp.stack(own_marks)
    other_marks = partner(jnp.stack(away_marks))

    def fetch_items(shard, copies, extra=(), extra_at=()):
        size = shard.shape[0]
        fixed = [fetched_from(shard, AXES, shift) for shift in (near, across)]
        held = swapped_with_all(copies, "z")
        free = [taken(held, z_at, 0, size) for _, z_at in forward[2:]]
        *free, fixed[0], fixed[1] = lax.optimization_barrier((*free, *fixed))
        y_steps, x_steps = zip(*[steps_to(at) for at, _ in [*forward[2:], *extra_at]])
        parts = stepped(stepped([*free, *extra], "y", y_steps), "x", x_steps)
        own = [*fixed, *parts[:2]]
        return own, [partner(value) for value in own], parts[2:]

    def fetch_users(shard, copies, marks, fixed_marks):
        size = shard.shape[0]
        direct = [fetched_from(shard, AXES, -near)]
        direct += [fetched_from(m, AXES, -shift) for m, shift in zip(fixed_marks, (near, across))]
        held = swapped_with_all(copies, ("x", "y"))
        pieces = [taken(held, at, 0, size) for at, _ in backward[1:]]
        moving = jnp.concatenate([*pieces[1:], *marks], axis=0)
        moving, *direct = lax.optimization_barrier((moving, *direct))
        held = swapped_with_all(jnp.broadcast_to(moving, (ring, *moving.shape)), "z")
        free = [taken(held, z_at, k * size, size) for k, (_, z_at) in enumerate(backward[2:])]
        moved = [taken(held, z_at, 2 * size + k * users, users) for k, (_, z_at) in enumerate(backward[2:])]
        own = [direct[0], pieces[0], *free]
        return own, [partner(value) for value in own], [*direct[1:], *moved]

    copies = jnp.broadcast_to(item_start, (ring, *item_start.shape))
    own, other, moved = fetch_items(item_start, copies, marks[2:], backward[2:])
    first_users, copies = solve_users(own, other, own_marks, other_marks, plane)

    own, other, moved = fetch_users(first_users, copies, moved, marks[:2])
    item_factors, copies = solve_items(own, other, moved, ring)

    own, other, _ = fetch_items(item_factors, copies)
    (user_factors,) = solve_users(own, other, own_marks, other_marks)
    return (user_factors, item_factors)


def solution(mesh):
    torus = Mesh(mesh.devices.reshape(4, 4, 8, 2), (*AXES, "grp"))
    everywhere = (*AXES, "grp")
    in_specs = (P(everywhere, None), P(None, AXES, "grp"), P(None, AXES), P())
    out_specs = (P(everywhere, None), P(everywhere, None))
    return jax.shard_map(body, mesh=torus, in_specs=in_specs, out_specs=out_specs, check_vma=False)
```

```python
import functools

import jax
import jax.numpy as jnp
from jax import lax
from jax.experimental import pallas as pl
from jax.experimental.pallas import tpu as pltpu
from jax.sharding import Mesh, PartitionSpec as P

SWEEPS = 4
RIDGE = 0.005
UNRATED = 64.0
RATED_BELOW = 32.0
AXES = ("x", "y", "z")
VMEM = pltpu.MemorySpace.VMEM
SMEM = pltpu.MemorySpace.SMEM


def split_parts(value):
    high = value.astype(jnp.bfloat16)
    low = (value - high.astype(jnp.float32)).astype(jnp.bfloat16)
    return jnp.concatenate([high, low], axis=0)


def dot_f32(a, b, dims=((1,), (0,))):
    return lax.dot_general(a, b, (dims, ((), ())), preferred_element_type=jnp.float32)


def relax(right, ridge, bound, rated, factors):
    rows = right.shape[0]
    inverse = 1.0 / bound
    answer = right * inverse
    for _ in range(SWEEPS - 1):
        inner = dot_f32(split_parts(answer), factors, ((1,), (1,)))
        inner = jnp.where(rated, inner[:rows] + inner[rows:], 0.0)
        outer = dot_f32(split_parts(inner), factors)
        applied = outer[:rows] + outer[rows:] + ridge * answer
        answer = answer + (right - applied) * inverse
    return answer.astype(jnp.bfloat16)


def users_kernel(*refs, pieces, copies):
    own, other = refs[:pieces], refs[pieces : 2 * pieces]
    own_marks_ref, other_marks_ref, *rest, factor_t_ref, mask_ref, sums_ref = refs[2 * pieces :]
    copies_ref = rest.pop() if copies else None
    (out_ref,) = rest
    rank = own[0].shape[1]
    rows = own_marks_ref.shape[1]
    parts = []
    half = own_marks_ref.shape[2]
    for k in range(pieces):
        for start in range(0, own[k].shape[0], half):
            parts += [own[k][start : start + half, :], other[k][start : start + half, :]]
    marks = []
    for k in range(own_marks_ref.shape[0]):
        marks += [own_marks_ref[k], other_marks_ref[k]]
    factors = jnp.concatenate(parts, axis=0)
    marked = jnp.concatenate(marks, axis=1).astype(jnp.float32)
    rated = jnp.abs(marked) < RATED_BELOW
    factor_t_ref[...] = factors.T
    mask = jnp.where(rated, 1.0, 0.0)
    mask_ref[...] = mask
    count = jnp.sum(mask, axis=1, keepdims=True)
    right = dot_f32(jnp.where(rated, marked, 0.0).astype(jnp.bfloat16), factors)
    together = 16

    def some(step, carry):
        chosen = mask_ref[pl.ds(step * together, together), :].astype(jnp.bfloat16)
        weighted = (factor_t_ref[...][None] * chosen[:, None, :]).reshape(together * rank, -1)
        gram = dot_f32(weighted, factors)
        total = jnp.sum(jnp.abs(gram).reshape(together, rank, rank), axis=1)
        sums_ref[pl.ds(step * together, together), :] = total
        return carry

    lax.fori_loop(0, rows // together, some, 0)
    ridge = RIDGE * (count + 1.0)
    bound = jnp.max(sums_ref[...], axis=1, keepdims=True) + ridge
    answer = relax(right, ridge, bound, rated, factors)
    out_ref[...] = answer
    for c in range(copies):
        copies_ref[c] = answer


def items_kernel(*refs):
    *ins, out_ref, copies_ref, sums_ref = refs
    own, other, marks = (ins[i * len(ins) // 3 : (i + 1) * len(ins) // 3] for i in range(3))
    rank = own[0].shape[1]
    items = out_ref.shape[0]
    parts = []
    for k in range(len(own)):
        parts += [own[k][...], other[k][...]]
    factors = jnp.concatenate(parts, axis=0)
    factor_t = factors.T
    marked = jnp.concatenate([ref[...].astype(jnp.float32) for ref in marks], axis=0).T
    rated = jnp.abs(marked) < RATED_BELOW
    mask = jnp.where(rated, 1.0, 0.0)
    count = jnp.sum(mask, axis=1, keepdims=True)
    right = dot_f32(jnp.where(rated, marked, 0.0).astype(jnp.bfloat16), factors)
    group = 8
    for j in range(items // group):
        row = mask[j * group : j * group + 1].astype(jnp.bfloat16)
        gram = dot_f32(factor_t * row, factors)
        total = jnp.sum(jnp.abs(gram), axis=0, keepdims=True)
        sums_ref[j * group : (j + 1) * group, :] = jnp.broadcast_to(total, (group, rank))
    ridge = RIDGE * (count + 1.0)
    bound = jnp.max(sums_ref[...], axis=1, keepdims=True) + ridge
    answer = relax(right, ridge, bound, rated, factors)
    out_ref[...] = answer
    for c in range(copies_ref.shape[0]):
        copies_ref[c] = answer


def vmem_specs(count):
    return [pl.BlockSpec(memory_space=VMEM)] * count


def solve_users(own, other, own_marks, other_marks, copies=0):
    tiles, rows, half = own_marks.shape
    rank = own[0].shape[1]
    width = tiles * 2 * half
    args = [*own, *other, own_marks, other_marks]
    shapes = [(rows, rank)]
    if copies:
        shapes.append((copies, rows, rank))
    return pl.pallas_call(
        functools.partial(users_kernel, pieces=len(own), copies=copies),
        out_shape=tuple(jax.ShapeDtypeStruct(shape, jnp.bfloat16) for shape in shapes),
        in_specs=vmem_specs(len(args)),
        out_specs=tuple(vmem_specs(len(shapes))),
        scratch_shapes=[
            pltpu.VMEM((rank, width), jnp.bfloat16),
            pltpu.VMEM((rows, width), jnp.float32),
            pltpu.VMEM((rows, rank), jnp.float32),
        ],
        name="users",
    )(*args)


def solve_items(own, other, marks, copies):
    rank = own[0].shape[1]
    items = marks[0].shape[1]
    args = [*own, *other, *marks]
    return pl.pallas_call(
        items_kernel,
        out_shape=(
            jax.ShapeDtypeStruct((items, rank), jnp.bfloat16),
            jax.ShapeDtypeStruct((copies, items, rank), jnp.bfloat16),
        ),
        in_specs=vmem_specs(len(args)),
        out_specs=tuple(vmem_specs(2)),
        scratch_shapes=[pltpu.VMEM((items, rank), jnp.float32)],
        name="items",
    )(*args)


def swapped_with_all(copies, axes):
    return lax.all_to_all(copies, axes, split_axis=0, concat_axis=0, tiled=True)


def fetched_from(value, axis, steps):
    count = 1
    for name in (axis if isinstance(axis, tuple) else (axis,)):
        count *= lax.axis_size(name)
    return lax.ppermute(value, axis, [((target + steps) % count, target) for target in range(count)])


def place_on(axis):
    return lax.axis_index(axis).astype(jnp.uint32)


def shift_digits(shift, z_first):
    ring, plane = lax.axis_size("z"), lax.axis_size(("x", "y"))
    z_bits = ring.bit_length() - 1
    z, z_shift = place_on("z"), shift & (ring - 1)
    carry = (z + z_shift) >> z_bits if z_first else (z < z_shift).astype(jnp.uint32)
    return (place_on(("x", "y")) + (shift >> z_bits) + carry) & (plane - 1), (z + z_shift) & (ring - 1)


def plane_steps(shift, z_first):
    ring, ny, nx = lax.axis_size("z"), lax.axis_size("y"), lax.axis_size("x")
    z_bits, y_bits = ring.bit_length() - 1, ny.bit_length() - 1
    z, y, z_shift = place_on("z"), place_on("y"), shift & (ring - 1)
    carry = (z + z_shift) >> z_bits if z_first else (z < z_shift).astype(jnp.uint32)
    y_sum = ((shift >> z_bits) & (ny - 1)) + carry
    x_shift = shift >> (z_bits + y_bits)
    y_step = y_sum & (ny - 1)
    y_then_x = (x_shift + ((y + y_sum) >> y_bits)) & (nx - 1)
    x_then_y = (x_shift + (y < y_sum).astype(jnp.uint32)) & (nx - 1)
    core = place_on("grp")
    return jnp.where(core == 0, y_step, x_then_y), jnp.where(core == 0, y_then_x, y_step)


def crossed_from(value, step, turn):
    names = (*AXES, "grp")
    nx, ny, nz, cores = (lax.axis_size(name) for name in names)
    pairs = []
    for x in range(nx):
        for y in range(ny):
            for z in range(nz):
                for core in range(cores):
                    along_y = (core == 0) == (turn == 0)
                    x_from, y_from = (x, (y + step) % ny) if along_y else ((x + step) % nx, y)
                    index = lambda i, j: ((i * ny + j) * nz + z) * cores + core
                    pairs.append((index(x_from, y_from), index(x, y)))
    return lax.ppermute(value, names, pairs)


def stepped(parts, turn, steps):
    held = jnp.concatenate(parts, axis=0)
    arrived = [held] + [crossed_from(held, step, turn) for step in range(1, lax.axis_size("y"))]
    chosen, start = [], 0
    for part, own_step in zip(parts, steps):
        value = part
        for step in range(1, len(arrived)):
            value = jnp.where(own_step == step, arrived[step][start : start + part.shape[0]], value)
        chosen.append(value)
        start += part.shape[0]
    return chosen


def taken(source, index, start, size):
    zero = jnp.uint32(0)
    return lax.dynamic_slice(source, (index, zero + start, zero), (1, size, source.shape[2]))[0]


def body(item_start, ratings, rating_bits, plan):
    tiles, users, items = ratings.shape
    own_half = lax.axis_index("grp")
    blocks = lax.axis_size(AXES)
    plane = lax.axis_size(("x", "y"))
    ring = lax.axis_size("z")
    rows = users // 2
    partner = lambda value: fetched_from(value, "grp", 1)

    near, across = blocks - 1, blocks // 2
    offsets = [plan[k].astype(jnp.uint32) for k in range(tiles)]
    zero = jnp.uint32(0)

    def place(wanted):
        at = zero
        for k in range(1, tiles):
            at = jnp.where(offsets[k] == wanted, jnp.uint32(k), at)
        return at

    first, second = place(near), place(across)
    low, high = jnp.minimum(first, second), jnp.maximum(first, second)
    third = jnp.where(low > 0, zero, jnp.where(high > 1, jnp.uint32(1), jnp.uint32(2)))
    fourth = jnp.uint32(tiles * (tiles - 1) // 2) - first - second - third
    order = (first, second, third, fourth)

    def offset_at(k):
        value = offsets[0]
        for j in range(1, tiles):
            value = jnp.where(k == j, offsets[j], value)
        return value

    shifts = (jnp.uint32(near), jnp.uint32(across), offset_at(third), offset_at(fourth))
    forward = [shift_digits(shift, True) for shift in shifts]
    backward = [shift_digits(blocks - shift, False) for shift in shifts]

    bit_count = 32 // lax.axis_size("grp")
    item_bits = own_half * bit_count + lax.broadcasted_iota(jnp.int32, (1, 1, items), 2) // (items // bit_count)
    rated = (jnp.right_shift(rating_bits[:, :, None], item_bits) & 1) == 1
    marks = jnp.where(rated, ratings, jnp.asarray(UNRATED, ratings.dtype))
    own_row = place_on("grp") * rows
    cut = lambda k, at: lax.dynamic_slice(marks, (k, at, zero), (1, rows, items))[0]
    own_marks = [cut(k, own_row) for k in order]
    away_marks = [cut(k, rows - own_row) for k in order]
    marks = [jnp.concatenate(pair, axis=0) for pair in zip(own_marks, away_marks)]
    own_marks = jnp.stack(own_marks)
    other_marks = partner(jnp.stack(away_marks))

    def fetch_items(shard, copies, extra=()):
        size = shard.shape[0]
        fixed = [fetched_from(shard, AXES, shift) for shift in (near, across)]
        held = swapped_with_all(copies, "z")
        free = [taken(held, z_at, 0, size) for _, z_at in forward[2:]]
        *free, fixed[0], fixed[1] = lax.optimization_barrier((*free, *fixed))
        steps = [plane_steps(shift, True) for shift in shifts[2:]]
        steps += [plane_steps(blocks - shift, False) for shift in shifts[2 : 2 + len(extra)]]
        parts = [*free, *extra]
        for turn in (0, 1):
            parts = stepped(parts, turn, [step[turn] for step in steps])
        own = [*fixed, jnp.concatenate(parts[:2], axis=0)]
        return own, [partner(value) for value in own], parts[2:]

    def fetch_users(shard, copies, marks, fixed_marks):
        size = shard.shape[0]
        direct = [fetched_from(shard, AXES, -near)]
        direct += [fetched_from(m, AXES, -shift) for m, shift in zip(fixed_marks, (near, across))]
        held = swapped_with_all(copies, ("x", "y"))
        pieces = [taken(held, at, 0, size) for at, _ in backward[1:]]
        moving = jnp.concatenate([*pieces[1:], *marks], axis=0)
        moving, *direct = lax.optimization_barrier((moving, *direct))
        held = swapped_with_all(jnp.broadcast_to(moving, (ring, *moving.shape)), "z")
        free = [taken(held, z_at, k * size, size) for k, (_, z_at) in enumerate(backward[2:])]
        moved = [taken(held, z_at, 2 * size + k * users, users) for k, (_, z_at) in enumerate(backward[2:])]
        own = [direct[0], pieces[0], *free]
        return own, [partner(value) for value in own], [*direct[1:], *moved]

    copies = jnp.broadcast_to(item_start, (ring, *item_start.shape))
    own, other, moved = fetch_items(item_start, copies, marks[2:])
    first_users, copies = solve_users(own, other, own_marks, other_marks, plane)

    own, other, moved = fetch_users(first_users, copies, moved, marks[:2])
    item_factors, copies = solve_items(own, other, moved, ring)

    own, other, _ = fetch_items(item_factors, copies)
    (user_factors,) = solve_users(own, other, own_marks, other_marks)
    return (user_factors, item_factors)


def solution(mesh):
    torus = Mesh(mesh.devices.reshape(4, 4, 8, 2), (*AXES, "grp"))
    everywhere = (*AXES, "grp")
    in_specs = (P(everywhere, None), P(None, AXES, "grp"), P(None, AXES), P())
    out_specs = (P(everywhere, None), P(everywhere, None))
    return jax.shard_map(body, mesh=torus, in_specs=in_specs, out_specs=out_specs, check_vma=False)
```

```python
import functools

import jax
import jax.numpy as jnp
from jax import lax
from jax.experimental import pallas as pl
from jax.experimental.pallas import tpu as pltpu
from jax.sharding import Mesh, PartitionSpec as P


SWEEPS = 4
RIDGE = 0.005
UNRATED = 64.0
RATED_BELOW = 32.0
AXES = ("x", "y", "z")
VMEM = pltpu.MemorySpace.VMEM


def split_parts(value):
    high = value.astype(jnp.bfloat16)
    low = (value - high.astype(jnp.float32)).astype(jnp.bfloat16)
    return jnp.concatenate([high, low], axis=0)


def dot_f32(a, b, dims=((1,), (0,))):
    return lax.dot_general(a, b, (dims, ((), ())), preferred_element_type=jnp.float32)


def relax(right, ridge, bound, rated, factors):
    rows = right.shape[0]
    inverse = 1.0 / bound
    answer = right * inverse
    for _ in range(SWEEPS - 1):
        inner = dot_f32(split_parts(answer), factors, ((1,), (1,)))
        inner = jnp.where(rated, inner[:rows] + inner[rows:], 0.0)
        outer = dot_f32(split_parts(inner), factors)
        applied = outer[:rows] + outer[rows:] + ridge * answer
        answer = answer + (right - applied) * inverse
    return answer.astype(jnp.bfloat16)


def users_kernel(*refs, pieces, copies):
    own, other = refs[:pieces], refs[pieces : 2 * pieces]
    own_marks_ref, other_marks_ref, *rest, factor_t_ref, mask_ref, sums_ref = refs[2 * pieces :]
    copies_ref = rest.pop() if copies else None
    (out_ref,) = rest
    rank = own[0].shape[1]
    rows = own_marks_ref.shape[1]
    parts = []
    half = own_marks_ref.shape[2]
    for k in range(pieces):
        for start in range(0, own[k].shape[0], half):
            parts += [own[k][start : start + half, :], other[k][start : start + half, :]]
    marks = []
    for k in range(own_marks_ref.shape[0]):
        marks += [own_marks_ref[k], other_marks_ref[k]]
    factors = jnp.concatenate(parts, axis=0)
    marked = jnp.concatenate(marks, axis=1).astype(jnp.float32)
    rated = jnp.abs(marked) < RATED_BELOW
    factor_t_ref[...] = factors.T
    mask = jnp.where(rated, 1.0, 0.0)
    mask_ref[...] = mask
    count = jnp.sum(mask, axis=1, keepdims=True)
    right = dot_f32(jnp.where(rated, marked, 0.0).astype(jnp.bfloat16), factors)
    together = 16

    def some(step, carry):
        chosen = mask_ref[pl.ds(step * together, together), :].astype(jnp.bfloat16)
        weighted = (factor_t_ref[...][None] * chosen[:, None, :]).reshape(together * rank, -1)
        gram = dot_f32(weighted, factors)
        total = jnp.sum(jnp.abs(gram).reshape(together, rank, rank), axis=1)
        sums_ref[pl.ds(step * together, together), :] = total
        return carry

    lax.fori_loop(0, rows // together, some, 0)
    ridge = RIDGE * (count + 1.0)
    bound = jnp.max(sums_ref[...], axis=1, keepdims=True) + ridge
    answer = relax(right, ridge, bound, rated, factors)
    out_ref[...] = answer
    for c in range(copies):
        copies_ref[c] = answer


def items_kernel(*refs):
    *ins, out_ref, copies_ref, sums_ref = refs
    own, other, marks = (ins[i * len(ins) // 3 : (i + 1) * len(ins) // 3] for i in range(3))
    rank = own[0].shape[1]
    items = out_ref.shape[0]
    parts = []
    for k in range(len(own)):
        parts += [own[k][...], other[k][...]]
    factors = jnp.concatenate(parts, axis=0)
    factor_t = factors.T
    marked = jnp.concatenate([ref[...].astype(jnp.float32) for ref in marks], axis=0).T
    rated = jnp.abs(marked) < RATED_BELOW
    mask = jnp.where(rated, 1.0, 0.0)
    count = jnp.sum(mask, axis=1, keepdims=True)
    right = dot_f32(jnp.where(rated, marked, 0.0).astype(jnp.bfloat16), factors)
    group = 8
    for j in range(items // group):
        row = mask[j * group : j * group + 1].astype(jnp.bfloat16)
        gram = dot_f32(factor_t * row, factors)
        total = jnp.sum(jnp.abs(gram), axis=0, keepdims=True)
        sums_ref[j * group : (j + 1) * group, :] = jnp.broadcast_to(total, (group, rank))
    ridge = RIDGE * (count + 1.0)
    bound = jnp.max(sums_ref[...], axis=1, keepdims=True) + ridge
    answer = relax(right, ridge, bound, rated, factors)
    out_ref[...] = answer
    for c in range(copies_ref.shape[0]):
        copies_ref[c] = answer


def vmem_specs(count):
    return [pl.BlockSpec(memory_space=VMEM)] * count


def solve_users(own, other, own_marks, other_marks, copies=0):
    tiles, rows, half = own_marks.shape
    rank = own[0].shape[1]
    width = tiles * 2 * half
    args = [*own, *other, own_marks, other_marks]
    shapes = [(rows, rank)]
    if copies:
        shapes.append((copies, rows, rank))
    return pl.pallas_call(
        functools.partial(users_kernel, pieces=len(own), copies=copies),
        out_shape=tuple(jax.ShapeDtypeStruct(shape, jnp.bfloat16) for shape in shapes),
        in_specs=vmem_specs(len(args)),
        out_specs=tuple(vmem_specs(len(shapes))),
        scratch_shapes=[
            pltpu.VMEM((rank, width), jnp.bfloat16),
            pltpu.VMEM((rows, width), jnp.float32),
            pltpu.VMEM((rows, rank), jnp.float32),
        ],
        name="users",
    )(*args)


def solve_items(own, other, marks, copies):
    rank = own[0].shape[1]
    items = marks[0].shape[1]
    args = [*own, *other, *marks]
    return pl.pallas_call(
        items_kernel,
        out_shape=(
            jax.ShapeDtypeStruct((items, rank), jnp.bfloat16),
            jax.ShapeDtypeStruct((copies, items, rank), jnp.bfloat16),
        ),
        in_specs=vmem_specs(len(args)),
        out_specs=tuple(vmem_specs(2)),
        scratch_shapes=[pltpu.VMEM((items, rank), jnp.float32)],
        name="items",
    )(*args)


def swapped_with_all(copies, axes):
    return lax.all_to_all(copies, axes, split_axis=0, concat_axis=0, tiled=True)


def fetched_from(value, axis, steps):
    count = 1
    for name in (axis if isinstance(axis, tuple) else (axis,)):
        count *= lax.axis_size(name)
    return lax.ppermute(value, axis, [((target + steps) % count, target) for target in range(count)])


def place_on(axis):
    return lax.axis_index(axis).astype(jnp.uint32)


def shift_digits(shift, z_first):
    ring, plane = lax.axis_size("z"), lax.axis_size(("x", "y"))
    z_bits = ring.bit_length() - 1
    z, z_shift = place_on("z"), shift & (ring - 1)
    carry = (z + z_shift) >> z_bits if z_first else (z < z_shift).astype(jnp.uint32)
    return (place_on(("x", "y")) + (shift >> z_bits) + carry) & (plane - 1), (z + z_shift) & (ring - 1)


def plane_steps(shift, z_first):
    ring, ny, nx = lax.axis_size("z"), lax.axis_size("y"), lax.axis_size("x")
    z_bits, y_bits = ring.bit_length() - 1, ny.bit_length() - 1
    z, y, z_shift = place_on("z"), place_on("y"), shift & (ring - 1)
    carry = (z + z_shift) >> z_bits if z_first else (z < z_shift).astype(jnp.uint32)
    y_sum = ((shift >> z_bits) & (ny - 1)) + carry
    x_shift = shift >> (z_bits + y_bits)
    y_step = y_sum & (ny - 1)
    y_then_x = (x_shift + ((y + y_sum) >> y_bits)) & (nx - 1)
    x_then_y = (x_shift + (y < y_sum).astype(jnp.uint32)) & (nx - 1)
    core = place_on("grp")
    return jnp.where(core == 0, y_step, x_then_y), jnp.where(core == 0, y_then_x, y_step)


def crossed_from(value, step, turn):
    names = (*AXES, "grp")
    nx, ny, nz, cores = (lax.axis_size(name) for name in names)
    pairs = []
    for x in range(nx):
        for y in range(ny):
            for z in range(nz):
                for core in range(cores):
                    along_y = (core == 0) == (turn == 0)
                    x_from, y_from = (x, (y + step) % ny) if along_y else ((x + step) % nx, y)
                    index = lambda i, j: ((i * ny + j) * nz + z) * cores + core
                    pairs.append((index(x_from, y_from), index(x, y)))
    return lax.ppermute(value, names, pairs)


def stepped(parts, turn, steps):
    held = jnp.concatenate(parts, axis=0)
    count = lax.axis_size("y")
    near_first = sorted(range(1, count), key=lambda step: min(step, count - step))
    arrivals = {step: crossed_from(held, step, turn) for step in near_first}
    arrived = [held] + [arrivals[step] for step in range(1, count)]
    chosen, start = [], 0
    for part, own_step in zip(parts, steps):
        value = part
        for step in range(1, len(arrived)):
            value = jnp.where(own_step == step, arrived[step][start : start + part.shape[0]], value)
        chosen.append(value)
        start += part.shape[0]
    return chosen


def taken(source, index, start, size):
    zero = jnp.uint32(0)
    return lax.dynamic_slice(source, (index, zero + start, zero), (1, size, source.shape[2]))[0]


def body(item_start, ratings, rating_bits, plan):
    tiles, users, items = ratings.shape
    own_half = lax.axis_index("grp")
    blocks = lax.axis_size(AXES)
    plane = lax.axis_size(("x", "y"))
    ring = lax.axis_size("z")
    rows = users // 2
    partner = lambda value: fetched_from(value, "grp", 1)

    near, across = blocks - 1, blocks // 2
    offsets = [plan[k].astype(jnp.uint32) for k in range(tiles)]
    zero = jnp.uint32(0)

    def place(wanted):
        at = zero
        for k in range(1, tiles):
            at = jnp.where(offsets[k] == wanted, jnp.uint32(k), at)
        return at

    first, second = place(near), place(across)
    low, high = jnp.minimum(first, second), jnp.maximum(first, second)
    third = jnp.where(low > 0, zero, jnp.where(high > 1, jnp.uint32(1), jnp.uint32(2)))
    fourth = jnp.uint32(tiles * (tiles - 1) // 2) - first - second - third
    order = (first, second, third, fourth)

    def offset_at(k):
        value = offsets[0]
        for j in range(1, tiles):
            value = jnp.where(k == j, offsets[j], value)
        return value

    shifts = (jnp.uint32(near), jnp.uint32(across), offset_at(third), offset_at(fourth))
    forward = [shift_digits(shift, True) for shift in shifts]
    backward = [shift_digits(blocks - shift, False) for shift in shifts]

    bit_count = 32 // lax.axis_size("grp")
    item_bits = own_half * bit_count + lax.broadcasted_iota(jnp.int32, (1, 1, items), 2) // (items // bit_count)
    rated = (jnp.right_shift(rating_bits[:, :, None], item_bits) & 1) == 1
    marks = jnp.where(rated, ratings, jnp.asarray(UNRATED, ratings.dtype))
    own_row = place_on("grp") * rows
    cut = lambda k, at: lax.dynamic_slice(marks, (k, at, zero), (1, rows, items))[0]
    own_marks = [cut(k, own_row) for k in order]
    away_marks = [cut(k, rows - own_row) for k in order]
    marks = [jnp.concatenate(pair, axis=0) for pair in zip(own_marks, away_marks)]
    own_marks = jnp.stack(own_marks)
    other_marks = partner(jnp.stack(away_marks))

    def fetch_items(shard, copies, extra=()):
        size = shard.shape[0]
        fixed = [fetched_from(shard, AXES, shift) for shift in (near, across)]
        held = swapped_with_all(copies, "z")
        free = [taken(held, z_at, 0, size) for _, z_at in forward[2:]]
        *free, fixed[0], fixed[1] = lax.optimization_barrier((*free, *fixed))
        steps = [plane_steps(shift, True) for shift in shifts[2:]]
        steps += [plane_steps(blocks - shift, False) for shift in shifts[2 : 2 + len(extra)]]
        parts = [*free, *extra]
        for turn in (0, 1):
            parts = stepped(parts, turn, [step[turn] for step in steps])
        own = [*fixed, jnp.concatenate(parts[:2], axis=0)]
        return own, [partner(value) for value in own], parts[2:]

    def fetch_users(shard, copies, marks, fixed_marks):
        size = shard.shape[0]
        direct = [fetched_from(shard, AXES, -near)]
        direct += [fetched_from(m, AXES, -shift) for m, shift in zip(fixed_marks, (near, across))]
        held = swapped_with_all(copies, ("x", "y"))
        pieces = [taken(held, at, 0, size) for at, _ in backward[1:]]
        moving = jnp.concatenate([*pieces[1:], *marks], axis=0)
        moving, *direct = lax.optimization_barrier((moving, *direct))
        held = swapped_with_all(jnp.broadcast_to(moving, (ring, *moving.shape)), "z")
        free = [taken(held, z_at, k * size, size) for k, (_, z_at) in enumerate(backward[2:])]
        moved = [taken(held, z_at, 2 * size + k * users, users) for k, (_, z_at) in enumerate(backward[2:])]
        own = [direct[0], pieces[0], *free]
        return own, [partner(value) for value in own], [*direct[1:], *moved]

    copies = jnp.broadcast_to(item_start, (ring, *item_start.shape))
    own, other, moved = fetch_items(item_start, copies, marks[2:])
    first_users, copies = solve_users(own, other, own_marks, other_marks, plane)

    own, other, moved = fetch_users(first_users, copies, moved, marks[:2])
    item_factors, copies = solve_items(own, other, moved, ring)

    own, other, _ = fetch_items(item_factors, copies)
    (user_factors,) = solve_users(own, other, own_marks, other_marks)
    return (user_factors, item_factors)


def solution(mesh):
    torus = Mesh(mesh.devices.reshape(4, 4, 8, 2), (*AXES, "grp"))
    everywhere = (*AXES, "grp")
    in_specs = (P(everywhere, None), P(None, AXES, "grp"), P(None, AXES), P())
    out_specs = (P(everywhere, None), P(everywhere, None))
    return jax.shard_map(body, mesh=torus, in_specs=in_specs, out_specs=out_specs, check_vma=False)
```

```python
import functools

import jax
import jax.numpy as jnp
from jax import lax
from jax.experimental import pallas as pl
from jax.experimental.pallas import tpu as pltpu
from jax.sharding import Mesh, PartitionSpec as P


SWEEPS = 4
RIDGE = 0.005
UNRATED = 64.0
RATED_BELOW = 32.0
AXES = ("x", "y", "z")
VMEM = pltpu.MemorySpace.VMEM


def split_parts(value):
    high = value.astype(jnp.bfloat16)
    low = (value - high.astype(jnp.float32)).astype(jnp.bfloat16)
    return jnp.concatenate([high, low], axis=0)


def dot_f32(a, b, dims=((1,), (0,))):
    return lax.dot_general(a, b, (dims, ((), ())), preferred_element_type=jnp.float32)


def relax(right, ridge, bound, rated, factors):
    rows = right.shape[0]
    inverse = 1.0 / bound
    answer = right * inverse
    for _ in range(SWEEPS - 1):
        inner = dot_f32(split_parts(answer), factors, ((1,), (1,)))
        inner = jnp.where(rated, inner[:rows] + inner[rows:], 0.0)
        outer = dot_f32(split_parts(inner), factors)
        applied = outer[:rows] + outer[rows:] + ridge * answer
        answer = answer + (right - applied) * inverse
    return answer.astype(jnp.bfloat16)


def users_kernel(*refs, pieces, copies):
    own, other = refs[:pieces], refs[pieces : 2 * pieces]
    own_marks_ref, other_marks_ref, *rest, factor_t_ref, mask_ref, sums_ref = refs[2 * pieces :]
    copies_ref = rest.pop() if copies else None
    (out_ref,) = rest
    rank = own[0].shape[1]
    rows = own_marks_ref.shape[1]
    parts = []
    half = own_marks_ref.shape[2]
    for k in range(pieces):
        for start in range(0, own[k].shape[0], half):
            parts += [own[k][start : start + half, :], other[k][start : start + half, :]]
    marks = []
    for k in range(own_marks_ref.shape[0]):
        marks += [own_marks_ref[k], other_marks_ref[k]]
    factors = jnp.concatenate(parts, axis=0)
    marked = jnp.concatenate(marks, axis=1).astype(jnp.float32)
    rated = jnp.abs(marked) < RATED_BELOW
    factor_t_ref[...] = factors.T
    mask = jnp.where(rated, 1.0, 0.0)
    mask_ref[...] = mask
    count = jnp.sum(mask, axis=1, keepdims=True)
    right = dot_f32(jnp.where(rated, marked, 0.0).astype(jnp.bfloat16), factors)
    together = 16

    def some(step, carry):
        chosen = mask_ref[pl.ds(step * together, together), :].astype(jnp.bfloat16)
        weighted = (factor_t_ref[...][None] * chosen[:, None, :]).reshape(together * rank, -1)
        gram = dot_f32(weighted, factors)
        total = jnp.sum(jnp.abs(gram).reshape(together, rank, rank), axis=1)
        sums_ref[pl.ds(step * together, together), :] = total
        return carry

    lax.fori_loop(0, rows // together, some, 0)
    ridge = RIDGE * (count + 1.0)
    bound = jnp.max(sums_ref[...], axis=1, keepdims=True) + ridge
    answer = relax(right, ridge, bound, rated, factors)
    out_ref[...] = answer
    for c in range(copies):
        copies_ref[c] = answer


def items_kernel(*refs):
    *ins, out_ref, copies_ref, sums_ref = refs
    own, other, marks = (ins[i * len(ins) // 3 : (i + 1) * len(ins) // 3] for i in range(3))
    rank = own[0].shape[1]
    items = out_ref.shape[0]
    parts = []
    for k in range(len(own)):
        parts += [own[k][...], other[k][...]]
    factors = jnp.concatenate(parts, axis=0)
    factor_t = factors.T
    marked = jnp.concatenate([ref[...].astype(jnp.float32) for ref in marks], axis=0).T
    rated = jnp.abs(marked) < RATED_BELOW
    mask = jnp.where(rated, 1.0, 0.0)
    count = jnp.sum(mask, axis=1, keepdims=True)
    right = dot_f32(jnp.where(rated, marked, 0.0).astype(jnp.bfloat16), factors)
    group = 8
    for j in range(items // group):
        row = mask[j * group : j * group + 1].astype(jnp.bfloat16)
        gram = dot_f32(factor_t * row, factors)
        total = jnp.sum(jnp.abs(gram), axis=0, keepdims=True)
        sums_ref[j * group : (j + 1) * group, :] = jnp.broadcast_to(total, (group, rank))
    ridge = RIDGE * (count + 1.0)
    bound = jnp.max(sums_ref[...], axis=1, keepdims=True) + ridge
    answer = relax(right, ridge, bound, rated, factors)
    out_ref[...] = answer
    for c in range(copies_ref.shape[0]):
        copies_ref[c] = answer


def vmem_specs(count):
    return [pl.BlockSpec(memory_space=VMEM)] * count


def solve_users(own, other, own_marks, other_marks, copies=0):
    tiles, rows, half = own_marks.shape
    rank = own[0].shape[1]
    width = tiles * 2 * half
    args = [*own, *other, own_marks, other_marks]
    shapes = [(rows, rank)]
    if copies:
        shapes.append((copies, rows, rank))
    return pl.pallas_call(
        functools.partial(users_kernel, pieces=len(own), copies=copies),
        out_shape=tuple(jax.ShapeDtypeStruct(shape, jnp.bfloat16) for shape in shapes),
        in_specs=vmem_specs(len(args)),
        out_specs=tuple(vmem_specs(len(shapes))),
        scratch_shapes=[
            pltpu.VMEM((rank, width), jnp.bfloat16),
            pltpu.VMEM((rows, width), jnp.float32),
            pltpu.VMEM((rows, rank), jnp.float32),
        ],
        name="users",
    )(*args)


def solve_items(own, other, marks, copies):
    rank = own[0].shape[1]
    items = marks[0].shape[1]
    args = [*own, *other, *marks]
    return pl.pallas_call(
        items_kernel,
        out_shape=(
            jax.ShapeDtypeStruct((items, rank), jnp.bfloat16),
            jax.ShapeDtypeStruct((copies, items, rank), jnp.bfloat16),
        ),
        in_specs=vmem_specs(len(args)),
        out_specs=tuple(vmem_specs(2)),
        scratch_shapes=[pltpu.VMEM((items, rank), jnp.float32)],
        name="items",
    )(*args)


def swapped_with_all(copies, axes):
    return lax.all_to_all(copies, axes, split_axis=0, concat_axis=0, tiled=True)


def fetched_from(value, axis, steps):
    count = 1
    for name in (axis if isinstance(axis, tuple) else (axis,)):
        count *= lax.axis_size(name)
    return lax.ppermute(value, axis, [((target + steps) % count, target) for target in range(count)])


def place_on(axis):
    return lax.axis_index(axis).astype(jnp.uint32)


def shift_digits(shift, z_first):
    ring, plane = lax.axis_size("z"), lax.axis_size(("x", "y"))
    z_bits = ring.bit_length() - 1
    z, z_shift = place_on("z"), shift & (ring - 1)
    carry = (z + z_shift) >> z_bits if z_first else (z < z_shift).astype(jnp.uint32)
    return (place_on(("x", "y")) + (shift >> z_bits) + carry) & (plane - 1), (z + z_shift) & (ring - 1)


def plane_steps(shift, z_first):
    ring, ny, nx = lax.axis_size("z"), lax.axis_size("y"), lax.axis_size("x")
    z_bits, y_bits = ring.bit_length() - 1, ny.bit_length() - 1
    z, y, z_shift = place_on("z"), place_on("y"), shift & (ring - 1)
    carry = (z + z_shift) >> z_bits if z_first else (z < z_shift).astype(jnp.uint32)
    y_sum = ((shift >> z_bits) & (ny - 1)) + carry
    x_shift = shift >> (z_bits + y_bits)
    y_step = y_sum & (ny - 1)
    y_then_x = (x_shift + ((y + y_sum) >> y_bits)) & (nx - 1)
    x_then_y = (x_shift + (y < y_sum).astype(jnp.uint32)) & (nx - 1)
    core = place_on("grp")
    return jnp.where(core == 0, y_step, x_then_y), jnp.where(core == 0, y_then_x, y_step)


def crossed_from(value, step, turn):
    names = (*AXES, "grp")
    nx, ny, nz, cores = (lax.axis_size(name) for name in names)
    pairs = []
    for x in range(nx):
        for y in range(ny):
            for z in range(nz):
                for core in range(cores):
                    along_y = (core == 0) == (turn == 0)
                    x_from, y_from = (x, (y + step) % ny) if along_y else ((x + step) % nx, y)
                    index = lambda i, j: ((i * ny + j) * nz + z) * cores + core
                    pairs.append((index(x_from, y_from), index(x, y)))
    return lax.ppermute(value, names, pairs)


def stepped(parts, turn, steps):
    held = jnp.concatenate(parts, axis=0)
    count = lax.axis_size("y")
    near_first = sorted(range(1, count), key=lambda step: min(step, count - step))
    arrivals = {step: crossed_from(held, step, turn) for step in near_first}
    arrived = [held] + [arrivals[step] for step in range(1, count)]
    chosen, start = [], 0
    for part, own_step in zip(parts, steps):
        value = part
        for step in range(1, len(arrived)):
            value = jnp.where(own_step == step, arrived[step][start : start + part.shape[0]], value)
        chosen.append(value)
        start += part.shape[0]
    return chosen


def taken(source, index, start, size):
    zero = jnp.uint32(0)
    return lax.dynamic_slice(source, (index, zero + start, zero), (1, size, source.shape[2]))[0]


def body(item_start, ratings, rating_bits, plan):
    tiles, users, items = ratings.shape
    own_half = lax.axis_index("grp")
    blocks = lax.axis_size(AXES)
    plane = lax.axis_size(("x", "y"))
    ring = lax.axis_size("z")
    rows = users // 2
    partner = lambda value: fetched_from(value, "grp", 1)

    near, across = blocks - 1, blocks // 2
    offsets = [plan[k].astype(jnp.uint32) for k in range(tiles)]
    zero = jnp.uint32(0)

    def place(wanted):
        at = zero
        for k in range(1, tiles):
            at = jnp.where(offsets[k] == wanted, jnp.uint32(k), at)
        return at

    first, second = place(near), place(across)
    low, high = jnp.minimum(first, second), jnp.maximum(first, second)
    third = jnp.where(low > 0, zero, jnp.where(high > 1, jnp.uint32(1), jnp.uint32(2)))
    fourth = jnp.uint32(tiles * (tiles - 1) // 2) - first - second - third
    order = (first, second, third, fourth)

    def offset_at(k):
        value = offsets[0]
        for j in range(1, tiles):
            value = jnp.where(k == j, offsets[j], value)
        return value

    shifts = (jnp.uint32(near), jnp.uint32(across), offset_at(third), offset_at(fourth))
    forward = [shift_digits(shift, True) for shift in shifts]
    backward = [shift_digits(blocks - shift, False) for shift in shifts]

    bit_count = 32 // lax.axis_size("grp")
    item_bits = own_half * bit_count + lax.broadcasted_iota(jnp.int32, (1, 1, items), 2) // (items // bit_count)
    rated = (jnp.right_shift(rating_bits[:, :, None], item_bits) & 1) == 1
    marks = jnp.where(rated, ratings, jnp.asarray(UNRATED, ratings.dtype))
    own_row = place_on("grp") * rows
    cut = lambda k, at: lax.dynamic_slice(marks, (k, at, zero), (1, rows, items))[0]
    own_marks = [cut(k, own_row) for k in order]
    away_marks = [cut(k, rows - own_row) for k in order]
    marks = [jnp.concatenate(pair, axis=0) for pair in zip(own_marks, away_marks)]
    own_marks = jnp.stack(own_marks)
    other_marks = partner(jnp.stack(away_marks))

    def fetch_items(shard, copies, extra=()):
        size = shard.shape[0]
        fixed = [fetched_from(shard, AXES, shift) for shift in (near, across)]
        held = swapped_with_all(copies, "z")
        free = [taken(held, z_at, 0, size) for _, z_at in forward[2:]]
        *free, fixed[0], fixed[1] = lax.optimization_barrier((*free, *fixed))
        steps = [plane_steps(shift, True) for shift in shifts[2:]]
        steps += [plane_steps(blocks - shift, False) for shift in shifts[2 : 2 + len(extra)]]
        parts = [*free, *extra]
        for turn in (0, 1):
            parts = stepped(parts, turn, [step[turn] for step in steps])
        own = [*fixed, jnp.concatenate(parts[:2], axis=0)]
        return own, [partner(value) for value in own], parts[2:]

    def fetch_users(shard, copies, marks, fixed_marks):
        size = shard.shape[0]
        near_marks, across_marks = lax.optimization_barrier((*fixed_marks, shard))[:2]
        direct = [fetched_from(jnp.concatenate([shard, near_marks], axis=0), AXES, -near)]
        direct += [fetched_from(across_marks, AXES, -across)]
        held = swapped_with_all(copies, ("x", "y"))
        pieces = [taken(held, at, 0, size) for at, _ in backward[1:]]
        moving = jnp.concatenate([*pieces[1:], *marks], axis=0)
        moving, *direct = lax.optimization_barrier((moving, *direct))
        held = swapped_with_all(jnp.broadcast_to(moving, (ring, *moving.shape)), "z")
        free = [taken(held, z_at, k * size, size) for k, (_, z_at) in enumerate(backward[2:])]
        moved = [taken(held, z_at, 2 * size + k * users, users) for k, (_, z_at) in enumerate(backward[2:])]
        own = [direct[0][:size], pieces[0], *free]
        return own, [partner(value) for value in own], [direct[0][size:], direct[1], *moved]

    copies = jnp.broadcast_to(item_start, (ring, *item_start.shape))
    own, other, moved = fetch_items(item_start, copies, marks[2:])
    first_users, copies = solve_users(own, other, own_marks, other_marks, plane)

    own, other, moved = fetch_users(first_users, copies, moved, marks[:2])
    item_factors, copies = solve_items(own, other, moved, ring)

    own, other, _ = fetch_items(item_factors, copies)
    (user_factors,) = solve_users(own, other, own_marks, other_marks)
    return (user_factors, item_factors)


def solution(mesh):
    torus = Mesh(mesh.devices.reshape(4, 4, 8, 2), (*AXES, "grp"))
    everywhere = (*AXES, "grp")
    in_specs = (P(everywhere, None), P(None, AXES, "grp"), P(None, AXES), P())
    out_specs = (P(everywhere, None), P(everywhere, None))
    return jax.shard_map(body, mesh=torus, in_specs=in_specs, out_specs=out_specs, check_vma=False)
```
